128 devices in a mesh: lat: 2 (over core), lev: 64 (over z, y, x).
Axes of the slice: x: 4, y: 4, z: 4, core: 2. Of those that a mesh axis runs over, the one named last changes fastest.
Arguments:
- potential_temp: float32 [16, 128, 5760], P('lat', 'lev'), may hold values from 0.5 to 2
- layer_thickness: float32 [16, 128, 5760], P('lat', 'lev'), as said below
- zonal_wind: float32 [16, 128, 5760], P('lat', 'lev'), may hold values from -6 to 6
- meridional_wind: float32 [16, 128, 5760], P('lat', 'lev'), may hold values from -6 to 6
- surface_height: float32 [16, 5760], P('lat'), may hold values from 0 to 2
- target_eta: float32 [129], replicated, may hold values from 0 to 1, as said below
- intersection: int32 [3, 2, 128, 2, 64], P(None, None, None, 'lat', 'lev'), may hold values from 0 to 127, as said below
Outputs:
- remapped_temp: float32 [16, 128, 5760], P('lat', 'lev')
- remapped_thickness: float32 [16, 128, 5760], P('lat', 'lev')
- remapped_zonal: float32 [16, 128, 5760], P('lat', 'lev')
- remapped_meridional: float32 [16, 128, 5760], P('lat', 'lev')
- geopotential: float32 [16, 128, 5760], P('lat', 'lev')
The draws below stay inside these ranges and needn't reach their ends.
Inputs may be any that keep to these rules, and one draw needn't show every extreme that they name: `layer_thickness`: every entry is positive. `target_eta`: strictly increasing, 0 at index 0 and 1 at index 128. intersection[kind, 0, k, b, c] is the first and intersection[kind, 1, k, b, c] the number of consecutive source layers that contain every source layer intersecting target layer k, in every column of block (b, c): latitude rows b * 8 to (b + 1) * 8 - 1 and longitudes c * 90 to (c + 1) * 90 - 1, for the edge set of that kind. Counts run from 1 to 3, and 3 is reached in every block; first plus count never exceeds 128.
All inputs are finite; a program needn't handle non-finite values.
Results may differ from the reference program's by a relative error of at most 0.0003.
Values sent between devices are 32-bit elements; how exact they have to be, the bound alone decides.
A program may use at most 128 MiB of HBM per device.

```python
import jax
import jax.numpy as jnp
from jax import lax

LEV = 128
LON = 5760
LAT_DEV = 8
WINDOW = 3
LAT = 16
LON_BLK = 90


def layer_counts(key):
    levels = LEV
    pair_count = levels // 2
    rising = levels // 4
    shifts = jnp.concatenate([jnp.ones((rising,), jnp.int32), -jnp.ones((rising + 1,), jnp.int32), jnp.zeros((levels - 2 * rising - 1,), jnp.int32)])
    shifts = jax.random.permutation(jax.random.fold_in(key, 11), shifts)
    block_rows = LAT // LAT_DEV
    blocks = LON // LON_BLK
    swapped = jax.random.randint(jax.random.fold_in(key, 12), (block_rows, blocks, pair_count), 0, 2)
    paired = shifts.reshape(pair_count, 2)
    leading = jnp.where(swapped == 1, paired[:, 1], paired[:, 0])
    second = jnp.where(swapped == 1, paired[:, 0], paired[:, 1])
    return 1 + jnp.stack([leading, second], axis=-1).reshape(block_rows, blocks, levels)


def target_levels(key):
    spacing = jax.random.uniform(jax.random.fold_in(key, 21), (LEV,), jnp.float32, 0.5, 1.5)
    running = jnp.cumsum(spacing)
    return jnp.concatenate([jnp.zeros((1,), jnp.float32), running[:-1] / running[-1], jnp.ones((1,), jnp.float32)])


def draw_target_eta(key, part):
    return target_levels(key)


def draw_intersection(key, part):
    counts = layer_counts(key)
    starts = jnp.cumsum(counts, axis=-1) - counts
    ending = starts + counts
    south_start = jnp.concatenate([starts[:1], starts[:-1]], 0)
    south_end = jnp.concatenate([ending[:1], ending[:-1]], 0)
    west_start = jnp.roll(starts, 1, axis=1)
    west_end = jnp.roll(ending, 1, axis=1)
    windows = [(starts, ending), (jnp.minimum(starts, south_start), jnp.maximum(ending, south_end)), (jnp.minimum(starts, west_start), jnp.maximum(ending, west_end))]
    table = jnp.stack([jnp.stack([lower, upper - lower + 1], 0) for lower, upper in windows], 0)
    return jnp.transpose(table, (0, 1, 4, 2, 3)).astype(jnp.int32)


def draw_layer_thickness(key, part):
    counts = layer_counts(key)
    levels = LEV
    target = target_levels(key)
    layer_end = jnp.cumsum(counts, axis=-1)
    edge_ids = jnp.arange(1, levels, dtype=jnp.int32)
    holder = jnp.sum((layer_end[..., None, :] < edge_ids[:, None]).astype(jnp.int32), axis=-1)
    holder_end = jnp.take_along_axis(layer_end, holder, axis=-1)
    holder_count = jnp.take_along_axis(counts, holder, axis=-1)
    rank_inside = edge_ids - 1 - (holder_end - holder_count)

    def spread(table):
        moved = jnp.transpose(table, (0, 2, 1))
        return jnp.repeat(jnp.repeat(moved, LAT_DEV, axis=0), LON_BLK, axis=2)
    holder_col = spread(holder)
    rank_col = spread(rank_inside).astype(jnp.float32)
    count_col = spread(holder_count).astype(jnp.float32)
    uniform_draw = jax.random.uniform(jax.random.fold_in(key, 31), holder_col.shape, jnp.float32)
    fraction = (rank_col + 0.15 + 0.7 * uniform_draw) / count_col
    surface_span = jax.random.uniform(jax.random.fold_in(key, 32), (LAT, LON), jnp.float32, 60.0, 104.0)
    upper_eta = jnp.take(target, holder_col)
    lower_eta = jnp.take(target, holder_col + 1)
    source_eta = upper_eta + fraction * (lower_eta - upper_eta)
    full_eta = jnp.concatenate([jnp.zeros((LAT, 1, LON), jnp.float32), source_eta, jnp.ones((LAT, 1, LON), jnp.float32)], 1)
    return surface_span[:, None, :] * (full_eta[:, 1:] - full_eta[:, :-1])


def block_scale(rng, shape, pieces, low, high):
    level = 1.0
    for position, shards_of in pieces:
        steps = jax.random.uniform(jax.random.fold_in(jax.random.fold_in(rng, 6), position), (shards_of,), jnp.float32, low / len(pieces), high / len(pieces))
        level = level * jnp.repeat(jnp.exp(steps), shape[position] // shards_of).reshape((-1,) + (1,) * (len(shape) - 1 - position))
    return level


def normal_values(rng, extent, deviation, most, pieces=(), held_as=jnp.bfloat16):
    result = jax.random.normal(rng, extent, jnp.float32) * deviation
    if len(pieces) > 0:
        result = block_scale(rng, extent, pieces, -0.22, 0.18) * result
    return jnp.clip(result, min=-most, max=most).astype(held_as)


def setup_inputs(seed: int = 0) -> dict:
    arg_keys = jax.random.split(jax.random.key(seed), 8)
    potential_temp = jnp.clip(0.5 + 1.5 * jax.random.uniform(arg_keys[0], (LAT, LEV, LON), jnp.float32) ** block_scale(arg_keys[0], (LAT, LEV, LON), ((0, 2), (1, 64)), -0.2, 0.2), 0.5, 2.0)
    layer_thickness = draw_layer_thickness(jax.random.fold_in(arg_keys[7], 71), 0)
    zonal_wind = normal_values(arg_keys[2], (LAT, LEV, LON), 1.0, 6.0, ((0, 2), (1, 64)), jnp.float32)
    meridional_wind = normal_values(arg_keys[3], (LAT, LEV, LON), 1.0, 6.0, ((0, 2), (1, 64)), jnp.float32)
    surface_height = jnp.clip(2.0 * jax.random.uniform(arg_keys[4], (LAT, LON), jnp.float32) ** block_scale(arg_keys[4], (LAT, LON), ((0, 2),), -0.2, 0.2), 0.0, 2.0)
    target_eta = draw_target_eta(jax.random.fold_in(arg_keys[7], 71), 0)
    intersection = draw_intersection(jax.random.fold_in(arg_keys[7], 71), 0)
    return dict(potential_temp=potential_temp, layer_thickness=layer_thickness, zonal_wind=zonal_wind, meridional_wind=meridional_wind, surface_height=surface_height, target_eta=target_eta, intersection=intersection)


pressure_top = 0.2
kappa_power = 0.2857


def piece_integral(left_edge, slope_term, curvature, lower_frac, upper_frac):
    span_one = upper_frac - lower_frac
    span_two = upper_frac * upper_frac - lower_frac * lower_frac
    span_three = upper_frac * upper_frac * upper_frac - lower_frac * lower_frac * lower_frac
    return left_edge * span_one + 0.5 * slope_term * span_two + curvature * (0.5 * span_two - span_three / 3.0)


def remap_row(values, edge_press, target_eta, starts, counts):
    layer_depth = edge_press[1:] - edge_press[:-1]
    interface = (layer_depth[1:] * values[:-1] + layer_depth[:-1] * values[1:]) / (layer_depth[:-1] + layer_depth[1:])
    left_edge = jnp.concatenate([values[:1], interface], 0)
    right_edge = jnp.concatenate([interface, values[-1:]], 0)
    slope_term = right_edge - left_edge
    curvature = 6.0 * (values - 0.5 * (left_edge + right_edge))
    surface_span = edge_press[-1:] - pressure_top
    target = pressure_top + target_eta[:, None] * surface_span
    target_depth = (target_eta[1:] - target_eta[:-1])[:, None] * surface_span
    levels = values.shape[0]
    accumulated = jnp.zeros_like(values)
    for offset in range(WINDOW):
        source_layer = jnp.clip(starts + offset, 0, levels - 1).astype(jnp.int32)
        source_top = jnp.take_along_axis(edge_press[:-1], source_layer, 0)
        source_depth = jnp.take_along_axis(layer_depth, source_layer, 0)
        lower_frac = jnp.clip((target[:-1] - source_top) / source_depth, 0.0, 1.0)
        upper_frac = jnp.clip((target[1:] - source_top) / source_depth, 0.0, 1.0)
        integral = piece_integral(jnp.take_along_axis(left_edge, source_layer, 0), jnp.take_along_axis(slope_term, source_layer, 0), jnp.take_along_axis(curvature, source_layer, 0), lower_frac, upper_frac)
        accumulated = accumulated + jnp.where(offset < counts, source_depth * integral, 0.0)
    return accumulated / target_depth, target_depth


def reference(potential_temp, layer_thickness, zonal_wind, meridional_wind, surface_height, target_eta, intersection):
    lat_rows = potential_temp.shape[0]
    zero_row = jnp.zeros_like(layer_thickness[:, :1])
    edge_press = pressure_top + jnp.concatenate([zero_row, jnp.cumsum(layer_thickness, axis=1)], 1)
    edge_power = jnp.power(edge_press, kappa_power)
    layer_work = potential_temp * (edge_power[:, 1:] - edge_power[:, :-1])
    geopotential = surface_height[:, None, :] + lax.cumsum(layer_work, axis=1, reverse=True)

    def one_row(row_index):
        own_edges = edge_press[row_index]
        south_edges = edge_press[jnp.maximum(row_index - 1, 0)]
        west_edges = jnp.roll(own_edges, 1, axis=1)
        block_table = intersection[:, :, :, row_index // LAT_DEV, :]
        windows = jnp.repeat(block_table, LON_BLK, axis=-1)
        new_temp, new_depth = remap_row(potential_temp[row_index], own_edges, target_eta, windows[0, 0], windows[0, 1])
        new_zonal, unused_one = remap_row(zonal_wind[row_index], 0.5 * (south_edges + own_edges), target_eta, windows[1, 0], windows[1, 1])
        new_merid, unused_two = remap_row(meridional_wind[row_index], 0.5 * (west_edges + own_edges), target_eta, windows[2, 0], windows[2, 1])
        return new_temp, new_depth, new_zonal, new_merid

    results = lax.map(one_row, jnp.arange(lat_rows, dtype=jnp.int32))
    return results[0], results[1], results[2], results[3], geopotential
```

```python
import functools

import jax
import jax.numpy as jnp
from jax import lax
from jax.experimental import pallas as pl
from jax.experimental.pallas import tpu as pltpu
from jax.sharding import PartitionSpec as P

TOP = 0.2
KAPPA = 0.2857
LEV = 128
LON = 5760
BLK = 90
N = 64
CHUNKS = LON // 128
STRIDE = 2 * CHUNKS
F32 = jnp.float32

FWD = ((1, 0, 0), (1, 1, 91), (0, 0, 182), (0, 1, 272), (2, 0, 384), (2, 1, 474), (3, 0, 564), (3, 1, 654))
FWD_REGS = 6
BACK = ((0, 0, 0), (0, 1, 90), (1, 0, 180), (2, 0, 270), (2, 1, 360), (3, 0, 450), (3, 1, 540), (4, 0, 630), (4, 1, 720))
BACK_REGS = 7


def lanes():
    return lax.broadcasted_iota(jnp.int32, (8, 128), 1)


def roll_lanes(x, shift):
    shift = shift % 128
    return x if shift == 0 else pltpu.roll(x, shift, axis=1)


def place(regs, piece, offset, width, lane):
    reg, start = divmod(offset, 128)
    regs[reg] = piece if regs[reg] is None else jnp.where(lane >= start, piece, regs[reg])
    if start + width > 128:
        regs[reg + 1] = piece


def take(load, offset, width, lane):
    reg, start = divmod(offset, 128)
    x = load(reg)
    if start + width > 128:
        x = jnp.where(lane >= start, x, load(reg + 1))
    return x


def pack_kernel(temp_ref, depth_ref, zonal_ref, merid_ref, out_ref):
    refs = (temp_ref, depth_ref, zonal_ref, merid_ref)
    lane = lanes()
    for c in range(N):
        regs = [None] * FWD_REGS
        for field, level, offset in FWD:
            extra = 1 if field == 1 else 0
            width = BLK + extra
            first = (BLK * c - extra) % LON
            chunk, start = divmod(first, 128)
            ref = refs[field]
            x = ref[pl.ds(2 * chunk + level, 8, stride=STRIDE), :]
            if start + width > 128:
                after = (chunk + 1) % CHUNKS
                y = ref[pl.ds(2 * after + level, 8, stride=STRIDE), :]
                x = jnp.where(lane >= start, x, y)
            place(regs, roll_lanes(x, offset - start), offset, width, lane)
        for r in range(FWD_REGS):
            out_ref[c, :, 128 * r : 128 * (r + 1)] = regs[r]


def compute_kernel(
    eta_ref, table_ref, recv_ref, partner_ref, out_ref,
    edge_ref, q_ref, rh_ref, c1_ref, c2_ref, c3_ref, res_ref,
):
    lane = lanes()
    row = lax.broadcasted_iota(jnp.int32, (8, 128), 0)
    lat = lax.axis_index("lat")
    own_first = jnp.logical_and(row == 0, lat == 0)
    top = jnp.full((8, 128), TOP, F32)
    for kind in range(3):
        edge_ref[kind, 0] = top

    def gather(s, carry):
        edge, south = carry

        def load(r):
            return recv_ref[s, :, 128 * r : 128 * (r + 1)]

        def load_south(r):
            theirs = partner_ref[s, :, 128 * r : 128 * (r + 1)]
            return jnp.where(row == 7, theirs, load(r))

        for field, level, offset in FWD:
            if field != 1:
                x = roll_lanes(take(load, offset, BLK, lane), -offset)
                q_ref[(0, 0, 1, 2)[field], 2 * s + level] = x
                continue
            x = roll_lanes(take(load, offset, BLK + 1, lane), -(offset + 1))
            y = roll_lanes(take(load_south, offset, BLK + 1, lane), -(offset + 1))
            y = jnp.where(own_first, x, pltpu.roll(y, 1, axis=0))
            edge = edge + x
            south = south + y
            at = 2 * s + level + 1
            edge_ref[0, at] = edge
            edge_ref[1, at] = 0.5 * (south + edge)
            edge_ref[2, at] = 0.5 * (roll_lanes(edge, 1) + edge)
        return edge, south

    last, _ = lax.fori_loop(0, N, gather, (top, top), unroll=2)

    def power(x):
        return jnp.exp(KAPPA * jnp.log(x))

    def integrate(t, carry):
        below, phi = carry
        s = LEV - 1 - t
        above = power(edge_ref[0, s])
        phi = phi + q_ref[0, s] * (below - above)
        res_ref[0, s] = phi
        return above, phi

    lax.fori_loop(0, LEV, integrate, (power(last), jnp.zeros((8, 128), F32)), unroll=4)

    for kind in range(3):

        def coefficients(s, left, right, q, edge, h):
            bend = q - 0.5 * (left + right)
            rh_ref[s] = 1.0 / h
            c1_ref[s] = h * left
            c2_ref[s] = h * (0.5 * (right - left) + 3.0 * bend)
            c3_ref[s] = -2.0 * (h * bend)

        def layer(s, carry):
            left, q, edge, h = carry
            lower = edge_ref[kind, s + 1]
            h_next = edge_ref[kind, s + 2] - lower
            q_next = q_ref[kind, s + 1]
            right = (h_next * q + h * q_next) / (h + h_next)
            coefficients(s, left, right, q, edge, h)
            return right, q_next, lower, h_next

        q0 = q_ref[kind, 0]
        h0 = edge_ref[kind, 1] - top
        left, q, edge, h = lax.fori_loop(0, LEV - 1, layer, (q0, q0, top, h0), unroll=4)
        coefficients(LEV - 1, left, q, q, edge, h)
        span = edge_ref[kind, LEV] - TOP

        def target(k, carry):
            upper = carry
            eta0, eta1 = eta_ref[k], eta_ref[k + 1]
            lower = TOP + eta1 * span
            start = table_ref[kind, 0, k]
            count = table_ref[kind, 1, k]
            total = jnp.zeros((8, 128), F32)
            for m in range(3):
                s = jnp.clip(start + m, 0, LEV - 1)
                weight = jnp.where(m < count, 1.0, 0.0).astype(F32)
                edge, rh = edge_ref[kind, s], rh_ref[s]
                c1, c2, c3 = c1_ref[s], c2_ref[s], c3_ref[s]
                x1 = jnp.clip((upper - edge) * rh, 0.0, 1.0)
                x2 = jnp.clip((lower - edge) * rh, 0.0, 1.0)
                share = x2 * (c1 + x2 * (c2 + x2 * c3)) - x1 * (c1 + x1 * (c2 + x1 * c3))
                total = total + weight * share
            res_ref[2 + kind, k] = total / ((eta1 - eta0) * span)
            return lower

        lax.fori_loop(0, LEV, target, TOP + eta_ref[0] * span, unroll=4)

    span = last - TOP

    def send(s, _):
        regs = [None] * BACK_REGS
        for field, level, offset in BACK:
            x = span if field == 1 else res_ref[field, 2 * s + level]
            place(regs, roll_lanes(x, offset), offset, BLK, lane)
        for r in range(BACK_REGS):
            out_ref[s, :, 128 * r : 128 * (r + 1)] = regs[r]
        return 0

    lax.fori_loop(0, N, send, 0, unroll=2)


def unpack_kernel(eta_ref, recv_ref, surface_ref, temp_ref, depth_ref, zonal_ref, merid_ref, phi_ref):
    lane = lanes()
    me = lax.axis_index("lev")
    steps = [eta_ref[2 * me + level + 1] - eta_ref[2 * me + level] for level in range(2)]
    for field, level, offset in BACK:
        current = None
        for c in range(N):

            def load(r):
                return recv_ref[c, :, 128 * r : 128 * (r + 1)]

            chunk, start = divmod(BLK * c, 128)
            x = roll_lanes(take(load, offset, BLK, lane), start - offset)
            current = x if start == 0 else jnp.where(lane >= start, x, current)
            if start + BLK < 128:
                continue
            if field == 1:
                for k in range(2):
                    depth_ref[pl.ds(2 * chunk + k, 8, stride=STRIDE), :] = steps[k] * current
            else:
                y = current
                if field == 0:
                    y = y + surface_ref[:, 128 * chunk : 128 * (chunk + 1)]
                ref = (phi_ref, None, temp_ref, zonal_ref, merid_ref)[field]
                ref[pl.ds(2 * chunk + level, 8, stride=STRIDE), :] = y
            current = x


def to_rows(x):
    return x.reshape(8, 2, CHUNKS, 128).transpose(0, 2, 1, 3).reshape(8 * STRIDE, 128)


def from_rows(x):
    return x.reshape(8, CHUNKS, 2, 128).transpose(0, 2, 1, 3).reshape(8, 2, LON)


VMEM = pl.BlockSpec(memory_space=pltpu.VMEM)
SMEM = pl.BlockSpec(memory_space=pltpu.SMEM)


def on_device(temp, depth, zonal, merid, surface, eta, intersection):
    table = intersection[:, :, :, 0, 0]
    packed = pl.pallas_call(
        pack_kernel,
        out_shape=jax.ShapeDtypeStruct((N, 8, 128 * FWD_REGS), F32),
        in_specs=[VMEM] * 4,
        out_specs=VMEM,
        name="pack",
    )(*(to_rows(x) for x in (temp, depth, zonal, merid)))
    recv = lax.all_to_all(packed, "lev", 0, 0, tiled=True)
    partner = lax.ppermute(recv[:, :, :256], "lat", [(0, 1), (1, 0)])
    block = pltpu.VMEM((LEV, 8, 128), F32)
    out = pl.pallas_call(
        compute_kernel,
        out_shape=jax.ShapeDtypeStruct((N, 8, 128 * BACK_REGS), F32),
        in_specs=[SMEM, SMEM, VMEM, VMEM],
        out_specs=VMEM,
        scratch_shapes=[
            pltpu.VMEM((3, LEV + 1, 8, 128), F32),
            pltpu.VMEM((3, LEV, 8, 128), F32),
            block, block, block, block,
            pltpu.VMEM((5, LEV, 8, 128), F32),
        ],
        name="remap",
    )(eta, table, recv, partner)
    back = lax.all_to_all(out, "lev", 0, 0, tiled=True)
    outs = pl.pallas_call(
        unpack_kernel,
        out_shape=[jax.ShapeDtypeStruct((8 * STRIDE, 128), F32)] * 5,
        in_specs=[SMEM, VMEM, VMEM],
        out_specs=[VMEM] * 5,
        name="unpack",
    )(eta, back, surface)
    return tuple(from_rows(x) for x in outs)


def solution(mesh):
    shards = P("lat", "lev", None)
    return jax.shard_map(
        on_device,
        mesh=mesh,
        in_specs=(shards,) * 4 + (P("lat", None), P(), P(None, None, None, "lat", "lev")),
        out_specs=(shards,) * 5,
        check_vma=False,
    )
```

```python
import functools

import jax
import jax.numpy as jnp
from jax import lax
from jax.experimental import pallas as pl
from jax.experimental.pallas import tpu as pltpu
from jax.sharding import PartitionSpec as P

TOP = 0.2
KAPPA = 0.2857
LEV = 128
LON = 5760
BLK = 90
N = 64
CHUNKS = LON // 128
F32 = jnp.float32

FWD = ((1, 0, 0), (1, 1, 91), (0, 0, 182), (0, 1, 272), (2, 0, 384), (2, 1, 474), (3, 0, 564), (3, 1, 654))
FWD_REGS = 6
BACK = ((0, 0, 0), (0, 1, 90), (1, 0, 180), (2, 0, 270), (2, 1, 360), (3, 0, 450), (3, 1, 540), (4, 0, 630), (4, 1, 720))
BACK_REGS = 7


def lanes():
    return lax.broadcasted_iota(jnp.int32, (8, 128), 1)


def roll_lanes(x, shift):
    shift = shift % 128
    return x if shift == 0 else pltpu.roll(x, shift, axis=1)


def place(regs, piece, offset, width, lane):
    reg, start = divmod(offset, 128)
    regs[reg] = piece if regs[reg] is None else jnp.where(lane >= start, piece, regs[reg])
    if start + width > 128:
        regs[reg + 1] = piece


def take(load, offset, width, lane):
    reg, start = divmod(offset, 128)
    x = load(reg)
    if start + width > 128:
        x = jnp.where(lane >= start, x, load(reg + 1))
    return x


def pack_kernel(temp_ref, depth_ref, zonal_ref, merid_ref, out_ref):
    refs = (temp_ref, depth_ref, zonal_ref, merid_ref)
    lane = lanes()
    for c in range(N):
        regs = [None] * FWD_REGS
        for field, level, offset in FWD:
            extra = 1 if field == 1 else 0
            width = BLK + extra
            first = (BLK * c - extra) % LON
            chunk, start = divmod(first, 128)
            ref = refs[field]
            x = ref[:, level, 128 * chunk : 128 * (chunk + 1)]
            if start + width > 128:
                after = (chunk + 1) % CHUNKS
                y = ref[:, level, 128 * after : 128 * (after + 1)]
                x = jnp.where(lane >= start, x, y)
            place(regs, roll_lanes(x, offset - start), offset, width, lane)
        for r in range(FWD_REGS):
            out_ref[c, :, 128 * r : 128 * (r + 1)] = regs[r]


def compute_kernel(
    eta_ref, table_ref, recv_ref, partner_ref, out_ref,
    edge_ref, q_ref, rh_ref, c1_ref, c2_ref, c3_ref, res_ref,
):
    lane = lanes()
    row = lax.broadcasted_iota(jnp.int32, (8, 128), 0)
    lat = lax.axis_index("lat")
    own_first = jnp.logical_and(row == 0, lat == 0)
    top = jnp.full((8, 128), TOP, F32)
    for kind in range(3):
        edge_ref[kind, 0] = top

    def gather(s, carry):
        edge, south = carry

        def load(r):
            return recv_ref[s, :, 128 * r : 128 * (r + 1)]

        def load_south(r):
            theirs = partner_ref[s, :, 128 * r : 128 * (r + 1)]
            return jnp.where(row == 7, theirs, load(r))

        for field, level, offset in FWD:
            if field != 1:
                x = roll_lanes(take(load, offset, BLK, lane), -offset)
                q_ref[(0, 0, 1, 2)[field], 2 * s + level] = x
                continue
            x = roll_lanes(take(load, offset, BLK + 1, lane), -(offset + 1))
            y = roll_lanes(take(load_south, offset, BLK + 1, lane), -(offset + 1))
            y = jnp.where(own_first, x, pltpu.roll(y, 1, axis=0))
            edge = edge + x
            south = south + y
            at = 2 * s + level + 1
            edge_ref[0, at] = edge
            edge_ref[1, at] = 0.5 * (south + edge)
            edge_ref[2, at] = 0.5 * (roll_lanes(edge, 1) + edge)
        return edge, south

    last, _ = lax.fori_loop(0, N, gather, (top, top), unroll=2)

    def power(x):
        return jnp.exp(KAPPA * jnp.log(x))

    def integrate(t, carry):
        below, phi = carry
        s = LEV - 1 - t
        above = power(edge_ref[0, s])
        phi = phi + q_ref[0, s] * (below - above)
        res_ref[0, s] = phi
        return above, phi

    lax.fori_loop(0, LEV, integrate, (power(last), jnp.zeros((8, 128), F32)), unroll=4)

    for kind in range(3):

        def coefficients(s, left, right, q, edge, h):
            bend = q - 0.5 * (left + right)
            rh_ref[s] = 1.0 / h
            c1_ref[s] = h * left
            c2_ref[s] = h * (0.5 * (right - left) + 3.0 * bend)
            c3_ref[s] = -2.0 * (h * bend)

        def layer(s, carry):
            left, q, edge, h = carry
            lower = edge_ref[kind, s + 1]
            h_next = edge_ref[kind, s + 2] - lower
            q_next = q_ref[kind, s + 1]
            right = (h_next * q + h * q_next) / (h + h_next)
            coefficients(s, left, right, q, edge, h)
            return right, q_next, lower, h_next

        q0 = q_ref[kind, 0]
        h0 = edge_ref[kind, 1] - top
        left, q, edge, h = lax.fori_loop(0, LEV - 1, layer, (q0, q0, top, h0), unroll=4)
        coefficients(LEV - 1, left, q, q, edge, h)
        span = edge_ref[kind, LEV] - TOP

        def target(k, carry):
            upper = carry
            eta0, eta1 = eta_ref[k], eta_ref[k + 1]
            lower = TOP + eta1 * span
            start = table_ref[kind, 0, k]
            count = table_ref[kind, 1, k]
            total = jnp.zeros((8, 128), F32)
            for m in range(3):
                s = jnp.clip(start + m, 0, LEV - 1)
                weight = jnp.where(m < count, 1.0, 0.0).astype(F32)
                edge, rh = edge_ref[kind, s], rh_ref[s]
                c1, c2, c3 = c1_ref[s], c2_ref[s], c3_ref[s]
                x1 = jnp.clip((upper - edge) * rh, 0.0, 1.0)
                x2 = jnp.clip((lower - edge) * rh, 0.0, 1.0)
                share = x2 * (c1 + x2 * (c2 + x2 * c3)) - x1 * (c1 + x1 * (c2 + x1 * c3))
                total = total + weight * share
            res_ref[2 + kind, k] = total / ((eta1 - eta0) * span)
            return lower

        lax.fori_loop(0, LEV, target, TOP + eta_ref[0] * span, unroll=4)

    span = last - TOP

    def send(s, _):
        regs = [None] * BACK_REGS
        for field, level, offset in BACK:
            x = span if field == 1 else res_ref[field, 2 * s + level]
            place(regs, roll_lanes(x, offset), offset, BLK, lane)
        for r in range(BACK_REGS):
            out_ref[s, :, 128 * r : 128 * (r + 1)] = regs[r]
        return 0

    lax.fori_loop(0, N, send, 0, unroll=2)


def unpack_kernel(eta_ref, recv_ref, surface_ref, temp_ref, depth_ref, zonal_ref, merid_ref, phi_ref):
    lane = lanes()
    me = lax.axis_index("lev")
    steps = [eta_ref[2 * me + level + 1] - eta_ref[2 * me + level] for level in range(2)]
    for field, level, offset in BACK:
        current = None
        for c in range(N):

            def load(r):
                return recv_ref[c, :, 128 * r : 128 * (r + 1)]

            chunk, start = divmod(BLK * c, 128)
            x = roll_lanes(take(load, offset, BLK, lane), start - offset)
            current = x if start == 0 else jnp.where(lane >= start, x, current)
            if start + BLK < 128:
                continue
            if field == 1:
                for k in range(2):
                    depth_ref[:, k, 128 * chunk : 128 * (chunk + 1)] = steps[k] * current
            else:
                y = current
                if field == 0:
                    y = y + surface_ref[:, 128 * chunk : 128 * (chunk + 1)]
                ref = (phi_ref, None, temp_ref, zonal_ref, merid_ref)[field]
                ref[:, level, 128 * chunk : 128 * (chunk + 1)] = y
            current = x


VMEM = pl.BlockSpec(memory_space=pltpu.VMEM)
SMEM = pl.BlockSpec(memory_space=pltpu.SMEM)


def on_device(temp, depth, zonal, merid, surface, eta, intersection):
    table = intersection[:, :, :, 0, 0]
    packed = pl.pallas_call(
        pack_kernel,
        out_shape=jax.ShapeDtypeStruct((N, 8, 128 * FWD_REGS), F32),
        in_specs=[VMEM] * 4,
        out_specs=VMEM,
        name="pack",
    )(temp, depth, zonal, merid)
    recv = lax.all_to_all(packed, "lev", 0, 0, tiled=True)
    partner = lax.ppermute(recv[:, :, :256], "lat", [(0, 1), (1, 0)])
    block = pltpu.VMEM((LEV, 8, 128), F32)
    out = pl.pallas_call(
        compute_kernel,
        out_shape=jax.ShapeDtypeStruct((N, 8, 128 * BACK_REGS), F32),
        in_specs=[SMEM, SMEM, VMEM, VMEM],
        out_specs=VMEM,
        scratch_shapes=[
            pltpu.VMEM((3, LEV + 1, 8, 128), F32),
            pltpu.VMEM((3, LEV, 8, 128), F32),
            block, block, block, block,
            pltpu.VMEM((5, LEV, 8, 128), F32),
        ],
        name="remap",
    )(eta, table, recv, partner)
    back = lax.all_to_all(out, "lev", 0, 0, tiled=True)
    outs = pl.pallas_call(
        unpack_kernel,
        out_shape=[jax.ShapeDtypeStruct((8, 2, LON), F32)] * 5,
        in_specs=[SMEM, VMEM, VMEM],
        out_specs=[VMEM] * 5,
        name="unpack",
    )(eta, back, surface)
    return tuple(outs)


def solution(mesh):
    shards = P("lat", "lev", None)
    return jax.shard_map(
        on_device,
        mesh=mesh,
        in_specs=(shards,) * 4 + (P("lat", None), P(), P(None, None, None, "lat", "lev")),
        out_specs=(shards,) * 5,
        check_vma=False,
    )
```

```python
import functools

import jax
import jax.numpy as jnp
from jax import lax
from jax.experimental import pallas as pl
from jax.experimental.pallas import tpu as pltpu
from jax.sharding import PartitionSpec as P

TOP = 0.2
KAPPA = 0.2857
LEV = 128
LON = 5760
BLK = 90
N = 64
CHUNKS = LON // 128
F32 = jnp.float32

FWD_A = ((1, 0, 0), (1, 1, 91), (0, 0, 182), (0, 1, 272))
FWD_B = ((2, 0, 0), (2, 1, 90), (3, 0, 180), (3, 1, 270))
BACK_A = ((0, 0, 0), (0, 1, 90), (1, 0, 180), (1, 1, 270), (2, 0, 360))
BACK_B = ((3, 0, 0), (3, 1, 90), (4, 0, 180), (4, 1, 270))
REGS_F, REGS_A, REGS_B = 3, 4, 3
MESH = pl.DeviceIdType.MESH


def lanes():
    return lax.broadcasted_iota(jnp.int32, (8, 128), 1)


def roll_lanes(x, shift):
    shift = shift % 128
    return x if isinstance(shift, int) and shift == 0 else pltpu.roll(x, shift, axis=1)


def place(regs, piece, offset, width, lane):
    reg, start = divmod(offset, 128)
    regs[reg] = piece if regs[reg] is None else jnp.where(lane >= start, piece, regs[reg])
    if start + width > 128:
        regs[reg + 1] = piece


def take(load, offset, width, lane):
    reg, start = divmod(offset, 128)
    x = load(reg)
    if start + width > 128:
        x = jnp.where(lane >= start, x, load(reg + 1))
    return x


def main_kernel(
    eta_ref, table_ref, temp_ref, depth_ref, zonal_ref, merid_ref, back_a, back_b,
    send_a, send_b, land_a, land_b, south_ref, ret_a, ret_b,
    edge_ref, q_ref, par_ref, res_ref, send_sem, recv_sem, own_sem,
):
    lat, me = lax.axis_index("lat"), lax.axis_index("lev")
    lane = lanes()
    row = lax.broadcasted_iota(jnp.int32, (8, 128), 0)
    other = (1 - lat, me)

    def peer(k):
        o = lax.rem(27 * k, N)
        x = lax.rem(lax.rem(me, 4) + lax.rem(o, 4), 4)
        y = lax.rem(lax.rem(me // 4, 4) + lax.rem(o // 4, 4), 4)
        z = lax.rem(me // 16 + o // 16, 4)
        return 16 * z + 4 * y + x

    barrier = pltpu.get_barrier_semaphore()

    def greet(k, _):
        pl.semaphore_signal(barrier, inc=1, device_id=(lat, peer(k)), device_id_type=MESH)
        return 0

    lax.fori_loop(1, N, greet, 0)
    pl.semaphore_signal(barrier, inc=1, device_id=other, device_id_type=MESH)

    def copy(src, dst, i, device):
        return pltpu.make_async_remote_copy(
            src_ref=src, dst_ref=dst, send_sem=send_sem.at[i], recv_sem=recv_sem.at[i],
            device_id=device, device_id_type=MESH,
        )

    def scatter(src, dst, i):
        def start(k, _):
            p = peer(k)
            copy(src.at[p], dst.at[me], i, (lat, p)).start()
            return 0

        lax.fori_loop(1, N, start, 0)

    def everyone(src, dst, i):
        return copy(src.at[pl.ds(0, N - 1)], dst.at[pl.ds(0, N - 1)], i, other)

    refs = (temp_ref, depth_ref, zonal_ref, merid_ref)

    def pack(c, _):
        for pieces, out in ((FWD_A, send_a), (FWD_B, send_b)):
            regs = [None] * REGS_F
            for field, level, offset in pieces:
                extra = 1 if field == 1 else 0
                first = lax.rem(BLK * c - extra + LON, LON)
                chunk, start = first // 128, lax.rem(first, 128)
                after = lax.rem(chunk + 1, CHUNKS)
                x = refs[field][:, level, pl.ds(pl.multiple_of(128 * chunk, 128), 128)]
                y = refs[field][:, level, pl.ds(pl.multiple_of(128 * after, 128), 128)]
                x = jnp.where(lane >= start, x, y)
                x = pltpu.roll(x, lax.rem(offset % 128 - start + 128, 128), axis=1)
                place(regs, x, offset, BLK + extra, lane)
            for r in range(REGS_F):
                out[c, :, 128 * r : 128 * (r + 1)] = regs[r]
        return 0

    lax.fori_loop(0, N, pack, 0, unroll=2)
    pl.semaphore_wait(barrier, N)
    scatter(send_a, land_a, 0)
    scatter(send_b, land_b, 1)
    land_a[me] = send_a[me]
    land_b[me] = send_b[me]

    top = jnp.full((8, 128), TOP, F32)
    zero = jnp.zeros((8, 128), F32)
    for kind in range(3):
        edge_ref[kind, 0] = top
    for p in range(5):
        par_ref[LEV, p] = zero

    def piece(ref, s, offset, width, shift):
        def load(r):
            return ref[s, :, 128 * r : 128 * (r + 1)]

        return roll_lanes(take(load, offset, width, lane), shift - offset)

    everyone(send_a, land_a, 0).wait_recv()
    share = copy(land_a.at[:, :, pl.ds(0, 256)], south_ref, 4, other)
    share.start()

    def gather_a(s, edge):
        for field, level, offset in FWD_A:
            if field == 0:
                q_ref[0, 2 * s + level] = piece(land_a, s, offset, BLK, 0)
                continue
            edge = edge + piece(land_a, s, offset, BLK + 1, -1)
            at = 2 * s + level + 1
            edge_ref[0, at] = edge
            edge_ref[2, at] = 0.5 * (roll_lanes(edge, 1) + edge)
        return edge

    last = lax.fori_loop(0, N, gather_a, top, unroll=2)

    def power(x):
        return jnp.exp(KAPPA * jnp.log(x))

    def integrate(t, carry):
        below, phi = carry
        s = LEV - 1 - t
        above = power(edge_ref[0, s])
        phi = phi + q_ref[0, s] * (below - above)
        res_ref[0, s] = phi
        return above, phi

    lax.fori_loop(0, LEV, integrate, (power(last), zero), unroll=4)

    def remap(kind, slot):
        def coefficients(s, left, right, q, edge, h):
            bend = q - 0.5 * (left + right)
            par_ref[s, 0] = edge
            par_ref[s, 1] = 1.0 / h
            par_ref[s, 2] = h * left
            par_ref[s, 3] = h * (0.5 * (right - left) + 3.0 * bend)
            par_ref[s, 4] = -2.0 * (h * bend)

        def layer(s, carry):
            left, q, edge, h = carry
            lower = edge_ref[kind, s + 1]
            h_next = edge_ref[kind, s + 2] - lower
            q_next = q_ref[kind, s + 1]
            right = (h_next * q + h * q_next) / (h + h_next)
            coefficients(s, left, right, q, edge, h)
            return right, q_next, lower, h_next

        q0 = q_ref[kind, 0]
        h0 = edge_ref[kind, 1] - top
        left, q, edge, h = lax.fori_loop(0, LEV - 1, layer, (q0, q0, top, h0), unroll=4)
        coefficients(LEV - 1, left, q, q, edge, h)
        span = edge_ref[kind, LEV] - TOP

        def target(k, upper):
            eta0, eta1 = eta_ref[k], eta_ref[k + 1]
            lower = TOP + eta1 * span
            first = table_ref[kind, 0, k]
            count = table_ref[kind, 1, k]
            total = zero
            for m in range(3):
                s = jnp.where(m < count, first + m, LEV)
                edge, rh = par_ref[s, 0], par_ref[s, 1]
                c1, c2, c3 = par_ref[s, 2], par_ref[s, 3], par_ref[s, 4]
                x1 = jnp.clip((upper - edge) * rh, 0.0, 1.0)
                x2 = jnp.clip((lower - edge) * rh, 0.0, 1.0)
                total = total + (x2 * (c1 + x2 * (c2 + x2 * c3)) - x1 * (c1 + x1 * (c2 + x1 * c3)))
            res_ref[slot, k] = total / ((eta1 - eta0) * span)
            return lower

        lax.fori_loop(0, LEV, target, TOP + eta_ref[0] * span, unroll=4)

    def send_back(pieces, regs_of, out, span):
        def build(s, _):
            regs = [None] * regs_of
            for field, level, offset in pieces:
                x = span if field == 2 else res_ref[field, 2 * s + level]
                place(regs, roll_lanes(x, offset), offset, BLK, lane)
            for r in range(regs_of):
                out[s, :, 128 * r : 128 * (r + 1)] = regs[r]
            return 0

        lax.fori_loop(0, N, build, 0, unroll=2)

    remap(0, 1)
    send_back(BACK_A, REGS_A, ret_a, last - TOP)
    scatter(ret_a, back_a, 2)

    everyone(send_b, land_b, 1).wait_recv()
    share.wait_recv()
    own_first = jnp.logical_and(row == 0, lat == 0)

    def gather_b(s, south):
        for field, level, offset in FWD_B:
            q_ref[field - 1, 2 * s + level] = piece(land_b, s, offset, BLK, 0)
        for level, offset in ((0, 0), (1, 91)):
            south = south + piece(south_ref, s, offset, BLK + 1, -1)
            at = 2 * s + level + 1
            own = edge_ref[0, at]
            before = pltpu.roll(jnp.where(row == 7, south, own), 1, axis=0)
            edge_ref[1, at] = jnp.where(own_first, own, 0.5 * (before + own))
        return south

    lax.fori_loop(0, N, gather_b, top, unroll=2)
    remap(1, 3)
    remap(2, 4)
    send_back(BACK_B, REGS_B, ret_b, None)
    scatter(ret_b, back_b, 3)

    mine_a = pltpu.make_async_copy(ret_a.at[me], back_a.at[me], own_sem.at[0])
    mine_b = pltpu.make_async_copy(ret_b.at[me], back_b.at[me], own_sem.at[1])
    mine_a.start()
    mine_b.start()
    everyone(send_a, land_a, 0).wait_send()
    everyone(send_b, land_b, 1).wait_send()
    share.wait_send()
    mine_a.wait()
    mine_b.wait()
    everyone(ret_a, back_a, 2).wait()
    everyone(ret_b, back_b, 3).wait()


def unpack_kernel(eta_ref, back_a, back_b, surface_ref, temp_ref, depth_ref, zonal_ref, merid_ref, phi_ref):
    lane = lanes()
    me = lax.axis_index("lev")
    steps = [eta_ref[2 * me + level + 1] - eta_ref[2 * me + level] for level in range(2)]
    for field, level, offset in BACK_A + BACK_B:
        recv_ref = back_b if field > 2 else back_a
        current = None
        for c in range(N):

            def load(r):
                return recv_ref[c, :, 128 * r : 128 * (r + 1)]

            chunk, start = divmod(BLK * c, 128)
            x = roll_lanes(take(load, offset, BLK, lane), start - offset)
            current = x if start == 0 else jnp.where(lane >= start, x, current)
            if start + BLK < 128:
                continue
            if field == 2:
                for k in range(2):
                    depth_ref[:, k, 128 * chunk : 128 * (chunk + 1)] = steps[k] * current
            else:
                y = current
                if field == 0:
                    y = y + surface_ref[:, 128 * chunk : 128 * (chunk + 1)]
                ref = (phi_ref, temp_ref, None, zonal_ref, merid_ref)[field]
                ref[:, level, 128 * chunk : 128 * (chunk + 1)] = y
            current = x


VMEM = pl.BlockSpec(memory_space=pltpu.VMEM)
SMEM = pl.BlockSpec(memory_space=pltpu.SMEM)


def on_device(temp, depth, zonal, merid, surface, eta, intersection):
    table = intersection[:, :, :, 0, 0]
    block = (LEV, 8, 128)
    backs = pl.pallas_call(
        main_kernel,
        out_shape=[
            jax.ShapeDtypeStruct((N, 8, 128 * REGS_A), F32),
            jax.ShapeDtypeStruct((N, 8, 128 * REGS_B), F32),
        ],
        in_specs=[SMEM, SMEM] + [VMEM] * 4,
        out_specs=[pl.BlockSpec(memory_space=pl.ANY)] * 2,
        scratch_shapes=[
            *[pltpu.VMEM((N, 8, 128 * REGS_F), F32)] * 4,
            pltpu.VMEM((N, 8, 256), F32),
            pltpu.VMEM((N, 8, 128 * REGS_A), F32),
            pltpu.VMEM((N, 8, 128 * REGS_B), F32),
            pltpu.VMEM((3, LEV + 1, 8, 128), F32),
            pltpu.VMEM((3, *block), F32),
            pltpu.VMEM((LEV + 1, 5, 8, 128), F32),
            pltpu.VMEM((5, *block), F32),
            pltpu.SemaphoreType.DMA((5,)),
            pltpu.SemaphoreType.DMA((5,)),
            pltpu.SemaphoreType.DMA((2,)),
        ],
        compiler_params=pltpu.CompilerParams(collective_id=0, has_side_effects=True),
        name="remap",
    )(eta, table, temp, depth, zonal, merid)
    outs = pl.pallas_call(
        unpack_kernel,
        out_shape=[jax.ShapeDtypeStruct((8, 2, LON), F32)] * 5,
        in_specs=[SMEM, VMEM, VMEM, VMEM],
        out_specs=[VMEM] * 5,
        name="unpack",
    )(eta, *backs, surface)
    return tuple(outs)


def solution(mesh):
    shards = P("lat", "lev", None)
    return jax.shard_map(
        on_device,
        mesh=mesh,
        in_specs=(shards,) * 4 + (P("lat", None), P(), P(None, None, None, "lat", "lev")),
        out_specs=(shards,) * 5,
        check_vma=False,
    )
```

```python
import functools

import jax
import jax.numpy as jnp
from jax import lax
from jax.experimental import pallas as pl
from jax.experimental.pallas import tpu as pltpu
from jax.sharding import PartitionSpec as P

TOP = 0.2
KAPPA = 0.2857
LEV = 128
LON = 5760
BLK = 90
N = 64
CHUNKS = LON // 128
F32 = jnp.float32

FWD_A = ((1, 0, 0), (1, 1, 91), (0, 0, 182), (0, 1, 272))
FWD_B = ((2, 0, 0), (2, 1, 90), (3, 0, 180), (3, 1, 270))
BACK_A = ((0, 0, 0), (0, 1, 90), (1, 0, 180), (1, 1, 270), (2, 0, 360))
BACK_B = ((3, 0, 0), (3, 1, 90), (4, 0, 180), (4, 1, 270))
REGS_F, REGS_A, REGS_B = 3, 4, 3
MESH = pl.DeviceIdType.MESH


def offsets():
    every = [(x, y, z) for z in range(4) for y in range(4) for x in range(4)][1:]
    order = []
    for d in sorted(every, key=lambda d: -sum(min(v, 4 - v) for v in d)):
        for r in range(3):
            e = d[r:] + d[:r]
            for f in (e, tuple((4 - v) % 4 for v in e)):
                if f not in order:
                    order.append(f)
    return order


OFFSETS = offsets()


def lanes():
    return lax.broadcasted_iota(jnp.int32, (8, 128), 1)


def roll_lanes(x, shift):
    shift = shift % 128
    return x if isinstance(shift, int) and shift == 0 else pltpu.roll(x, shift, axis=1)


def place(regs, piece, offset, width, lane):
    reg, start = divmod(offset, 128)
    regs[reg] = piece if regs[reg] is None else jnp.where(lane >= start, piece, regs[reg])
    if start + width > 128:
        regs[reg + 1] = piece


def take(load, offset, width, lane):
    reg, start = divmod(offset, 128)
    x = load(reg)
    if start + width > 128:
        x = jnp.where(lane >= start, x, load(reg + 1))
    return x


def main_kernel(
    eta_ref, table_ref, temp_hbm, depth_hbm, zonal_hbm, merid_hbm, back_a, back_b,
    temp_ref, depth_ref, zonal_ref, merid_ref,
    send_a, send_b, land_a, land_b, south_ref, ret_a, ret_b,
    edge_ref, par_ref, res_ref, send_sem, recv_sem, own_sem,
):
    lat, me = lax.axis_index("lat"), lax.axis_index("lev")
    lane = lanes()
    row = lax.broadcasted_iota(jnp.int32, (8, 128), 0)
    other = (1 - lat, me)
    loads = [
        pltpu.make_async_copy(src, dst, own_sem.at[i])
        for i, (src, dst) in enumerate(
            ((depth_hbm, depth_ref), (temp_hbm, temp_ref), (zonal_hbm, zonal_ref), (merid_hbm, merid_ref))
        )
    ]
    for c in loads:
        c.start()

    along = [
        [step * lax.rem(at + d, 4) for d in range(4)]
        for step, at in ((1, lax.rem(me, 4)), (4, lax.rem(me // 4, 4)), (16, me // 16))
    ]
    peers = [along[0][x] + along[1][y] + along[2][z] for x, y, z in OFFSETS]
    barrier = pltpu.get_barrier_semaphore()
    for p in peers:
        pl.semaphore_signal(barrier, inc=1, device_id=(lat, p), device_id_type=MESH)
    pl.semaphore_signal(barrier, inc=1, device_id=other, device_id_type=MESH)

    def copy(src, dst, i, device):
        return pltpu.make_async_remote_copy(
            src_ref=src, dst_ref=dst, send_sem=send_sem.at[i], recv_sem=recv_sem.at[i],
            device_id=device, device_id_type=MESH,
        )

    def scatter(src, dst, i):
        for p in peers:
            copy(src.at[p], dst.at[me], i, (lat, p)).start()

    def everyone(src, dst, i):
        return copy(src.at[pl.ds(0, N - 1)], dst.at[pl.ds(0, N - 1)], i, other)

    refs = (temp_ref, depth_ref, zonal_ref, merid_ref)

    def pack(pieces, out):
        def one(c, _):
            regs = [None] * REGS_F
            for field, level, offset in pieces:
                extra = 1 if field == 1 else 0
                first = lax.rem(BLK * c - extra + LON, LON)
                chunk, start = first // 128, lax.rem(first, 128)
                after = lax.rem(chunk + 1, CHUNKS)
                x = refs[field][:, level, pl.ds(pl.multiple_of(128 * chunk, 128), 128)]
                y = refs[field][:, level, pl.ds(pl.multiple_of(128 * after, 128), 128)]
                x = jnp.where(lane >= start, x, y)
                x = pltpu.roll(x, lax.rem(offset % 128 - start + 128, 128), axis=1)
                place(regs, x, offset, BLK + extra, lane)
            for r in range(REGS_F):
                out[c, :, 128 * r : 128 * (r + 1)] = regs[r]
            return 0

        lax.fori_loop(0, N, one, 0, unroll=2)

    loads[0].wait()
    loads[1].wait()
    pack(FWD_A, send_a)
    land_a[me] = send_a[me]
    pl.semaphore_wait(barrier, N)
    scatter(send_a, land_a, 0)
    loads[2].wait()
    loads[3].wait()
    pack(FWD_B, send_b)
    land_b[me] = send_b[me]
    scatter(send_b, land_b, 1)

    top = jnp.full((8, 128), TOP, F32)
    zero = jnp.zeros((8, 128), F32)
    for kind in range(3):
        for p in range(6):
            par_ref[kind, LEV, p] = zero

    def piece(ref, s, offset, width, shift):
        def load(r):
            return ref[s, :, 128 * r : 128 * (r + 1)]

        return roll_lanes(take(load, offset, width, lane), shift - offset)

    def power(x):
        return jnp.exp(KAPPA * jnp.log(x))

    def coefficients(kind, s, above, left, right, q, edge, h):
        bend = q - 0.5 * (left + right)
        par_ref[kind, s, 0] = edge
        par_ref[kind, s, 1] = 1.0 / h
        par_ref[kind, s, 2] = h * left
        par_ref[kind, s, 3] = h * (0.5 * (right - left) + 3.0 * bend)
        par_ref[kind, s, 4] = -2.0 * (h * bend)
        par_ref[kind, s, 5] = above
        return above + h * q

    def layer(kind, s, state, edge_next, q_next, first):
        above, left, q, edge, h, lower = state
        h_next = edge_next - lower
        if first:
            return zero, q_next, q_next, lower, h_next, edge_next
        right = (h_next * q + h * q_next) / (h + h_next)
        above = coefficients(kind, s - 1, above, left, right, q, edge, h)
        return above, right, q_next, lower, h_next, edge_next

    def finish(kind, state):
        above, left, q, edge, h, lower = state
        coefficients(kind, LEV - 1, above, left, q, q, edge, h)
        return lower - TOP

    begin = (zero, zero, zero, zero, zero, top)

    everyone(send_a, land_a, 0).wait_recv()
    share = copy(land_a.at[:, :, pl.ds(0, 256)], south_ref, 4, other)
    share.start()

    def gather_a(s, carry, first=False):
        state, press, work = carry
        for level in range(2):
            x = piece(land_a, s, 91 * level, BLK + 1, -1)
            q = piece(land_a, s, 182 + 90 * level, BLK, 0)
            edge = state[5] + x
            state = layer(0, 2 * s + level, state, edge, q, first and level == 0)
            edge_ref[2 * s + level] = edge
            res_ref[0, 2 * s + level] = work
            below = power(edge)
            work = work + q * (below - press)
            press = below
        return state, press, work

    carry = gather_a(0, (begin, power(top), zero), True)
    state, _, work = lax.fori_loop(1, N, gather_a, carry, unroll=3)
    depth = finish(0, state)

    def remap(kinds, spans):
        def target(k, carry):
            eta0, eta1 = eta_ref[k], eta_ref[k + 1]
            out = []
            for kind, span, before in zip(kinds, spans, carry):
                lower = TOP + eta1 * span
                first = table_ref[kind, 0, k]
                count = table_ref[kind, 1, k]
                mass = par_ref[kind, first, 5]
                for m in range(3):
                    s = first if m == 0 else jnp.where(m < count, first + m, LEV)
                    x = jnp.clip((lower - par_ref[kind, s, 0]) * par_ref[kind, s, 1], 0.0, 1.0)
                    mass = mass + x * (par_ref[kind, s, 2] + x * (par_ref[kind, s, 3] + x * par_ref[kind, s, 4]))
                res_ref[1 + kind, k] = (mass - before) / ((eta1 - eta0) * span)
                out.append(mass)
            return tuple(out)

        lax.fori_loop(0, LEV, target, (zero,) * len(kinds), unroll=4)

    def send_back(pieces, regs_of, out):
        def build(s, _):
            regs = [None] * regs_of
            for field, level, offset in pieces:
                if field == 2:
                    x = depth
                else:
                    x = res_ref[(0, 1, None, 2, 3)[field], 2 * s + level]
                if field == 0:
                    x = work - x
                place(regs, roll_lanes(x, offset), offset, BLK, lane)
            for r in range(regs_of):
                out[s, :, 128 * r : 128 * (r + 1)] = regs[r]
            return 0

        lax.fori_loop(0, N, build, 0, unroll=4)

    mine_a = pltpu.make_async_copy(ret_a.at[me], back_a.at[me], own_sem.at[4])
    mine_b = pltpu.make_async_copy(ret_b.at[me], back_b.at[me], own_sem.at[5])
    remap((0,), (depth,))
    send_back(BACK_A, REGS_A, ret_a)
    scatter(ret_a, back_a, 2)
    mine_a.start()

    share.wait_recv()
    everyone(send_b, land_b, 1).wait_recv()
    own_first = jnp.logical_and(row == 0, lat == 0)

    def gather_b(s, carry, first=False):
        south, zonal, merid = carry
        for level in range(2):
            at = 2 * s + level
            south = south + piece(south_ref, s, 91 * level, BLK + 1, -1)
            own = edge_ref[at]
            before = pltpu.roll(jnp.where(row == 7, south, own), 1, axis=0)
            edge = jnp.where(own_first, own, 0.5 * (before + own))
            zonal = layer(1, at, zonal, edge, piece(land_b, s, 90 * level, BLK, 0), first and level == 0)
            edge = 0.5 * (roll_lanes(own, 1) + own)
            merid = layer(2, at, merid, edge, piece(land_b, s, 180 + 90 * level, BLK, 0), first and level == 0)
        return south, zonal, merid

    carry = gather_b(0, (top, begin, begin), True)
    _, zonal, merid = lax.fori_loop(1, N, gather_b, carry, unroll=3)
    remap((1, 2), (finish(1, zonal), finish(2, merid)))
    send_back(BACK_B, REGS_B, ret_b)
    scatter(ret_b, back_b, 3)
    mine_b.start()

    everyone(send_a, land_a, 0).wait_send()
    everyone(send_b, land_b, 1).wait_send()
    share.wait_send()
    mine_a.wait()
    mine_b.wait()
    everyone(ret_a, back_a, 2).wait()
    everyone(ret_b, back_b, 3).wait()


def unpack_kernel(
    eta_ref, hbm_a, hbm_b, surface_hbm, temp_hbm, depth_hbm, zonal_hbm, merid_hbm, phi_hbm,
    back_a, back_b, surface_ref, out_ref, in_sem, out_sem,
):
    lane = lanes()
    me = lax.axis_index("lev")
    steps = [eta_ref[2 * me + level + 1] - eta_ref[2 * me + level] for level in range(2)]
    loads = [
        pltpu.make_async_copy(src, dst, in_sem.at[i])
        for i, (src, dst) in enumerate(((surface_hbm, surface_ref), (hbm_a, back_a), (hbm_b, back_b)))
    ]
    for c in loads:
        c.start()
    outs = (phi_hbm, temp_hbm, depth_hbm, zonal_hbm, merid_hbm)
    stores = [pltpu.make_async_copy(out_ref.at[i], outs[i], out_sem.at[i]) for i in range(5)]
    loads[0].wait()
    loads[1].wait()
    for i, (field, level, offset) in enumerate(BACK_A + BACK_B):
        if i == len(BACK_A):
            loads[2].wait()
        recv_ref = back_b if field > 2 else back_a
        current = None
        for c in range(N):

            def load(r):
                return recv_ref[c, :, 128 * r : 128 * (r + 1)]

            chunk, start = divmod(BLK * c, 128)
            x = roll_lanes(take(load, offset, BLK, lane), start - offset)
            current = x if start == 0 else jnp.where(lane >= start, x, current)
            if start + BLK < 128:
                continue
            at = slice(128 * chunk, 128 * (chunk + 1))
            if field == 2:
                for k in range(2):
                    out_ref[2, :, k, at] = steps[k] * current
            else:
                y = current + surface_ref[:, at] if field == 0 else current
                out_ref[field, :, level, at] = y
            current = x
        if field == 2 or level == 1:
            stores[field].start()
    for c in stores:
        c.wait()


ANY = pl.BlockSpec(memory_space=pl.ANY)
SMEM = pl.BlockSpec(memory_space=pltpu.SMEM)


def on_device(temp, depth, zonal, merid, surface, eta, intersection):
    table = intersection[:, :, :, 0, 0]
    backs = pl.pallas_call(
        main_kernel,
        out_shape=[
            jax.ShapeDtypeStruct((N, 8, 128 * REGS_A), F32),
            jax.ShapeDtypeStruct((N, 8, 128 * REGS_B), F32),
        ],
        in_specs=[SMEM, SMEM] + [ANY] * 4,
        out_specs=[ANY] * 2,
        scratch_shapes=[
            *[pltpu.VMEM((8, 2, LON), F32)] * 4,
            *[pltpu.VMEM((N, 8, 128 * REGS_F), F32)] * 4,
            pltpu.VMEM((N, 8, 256), F32),
            pltpu.VMEM((N, 8, 128 * REGS_A), F32),
            pltpu.VMEM((N, 8, 128 * REGS_B), F32),
            pltpu.VMEM((LEV, 8, 128), F32),
            pltpu.VMEM((3, LEV + 1, 6, 8, 128), F32),
            pltpu.VMEM((4, LEV, 8, 128), F32),
            pltpu.SemaphoreType.DMA((5,)),
            pltpu.SemaphoreType.DMA((5,)),
            pltpu.SemaphoreType.DMA((6,)),
        ],
        compiler_params=pltpu.CompilerParams(collective_id=0, has_side_effects=True),
        name="remap",
    )(eta, table, temp, depth, zonal, merid)
    outs = pl.pallas_call(
        unpack_kernel,
        out_shape=[jax.ShapeDtypeStruct((8, 2, LON), F32)] * 5,
        in_specs=[SMEM, ANY, ANY, ANY],
        out_specs=[ANY] * 5,
        scratch_shapes=[
            pltpu.VMEM((N, 8, 128 * REGS_A), F32),
            pltpu.VMEM((N, 8, 128 * REGS_B), F32),
            pltpu.VMEM((8, LON), F32),
            pltpu.VMEM((5, 8, 2, LON), F32),
            pltpu.SemaphoreType.DMA((3,)),
            pltpu.SemaphoreType.DMA((5,)),
        ],
        name="unpack",
    )(eta, *backs, surface)
    return tuple(outs)


def solution(mesh):
    shards = P("lat", "lev", None)
    return jax.shard_map(
        on_device,
        mesh=mesh,
        in_specs=(shards,) * 4 + (P("lat", None), P(), P(None, None, None, "lat", "lev")),
        out_specs=(shards,) * 5,
        check_vma=False,
    )
```

```python
import functools

import jax
import jax.numpy as jnp
from jax import lax
from jax.experimental import pallas as pl
from jax.experimental.pallas import tpu as pltpu
from jax.sharding import PartitionSpec as P

TOP = 0.2
KAPPA = 0.2857
LEV = 128
LON = 5760
BLK = 90
N = 64
CHUNKS = LON // 128
F32 = jnp.float32

FWD_A = ((1, 0, 0), (1, 1, 91), (0, 0, 182), (0, 1, 272))
FWD_B = ((2, 0, 0), (2, 1, 90), (3, 0, 180), (3, 1, 270))
BACK_A = ((0, 0, 0), (0, 1, 90), (1, 0, 180), (1, 1, 270), (2, 0, 360))
BACK_B = ((3, 0, 0), (3, 1, 90), (4, 0, 180), (4, 1, 270))
REGS_F, REGS_A, REGS_B = 3, 4, 3
MESH = pl.DeviceIdType.MESH


def offsets():
    every = [(x, y, z) for z in range(4) for y in range(4) for x in range(4)][1:]
    order = []
    for d in sorted(every, key=lambda d: -sum(min(v, 4 - v) for v in d)):
        for r in range(3):
            e = d[r:] + d[:r]
            for f in (e, tuple((4 - v) % 4 for v in e)):
                if f not in order:
                    order.append(f)
    return order


OFFSETS = offsets()


def lanes():
    return lax.broadcasted_iota(jnp.int32, (8, 128), 1)


def roll_lanes(x, shift):
    shift = shift % 128
    return x if isinstance(shift, int) and shift == 0 else pltpu.roll(x, shift, axis=1)


def place(regs, piece, offset, width, lane):
    reg, start = divmod(offset, 128)
    regs[reg] = piece if regs[reg] is None else jnp.where(lane >= start, piece, regs[reg])
    if start + width > 128:
        regs[reg + 1] = piece


def take(load, offset, width, lane):
    reg, start = divmod(offset, 128)
    x = load(reg)
    if start + width > 128:
        x = jnp.where(lane >= start, x, load(reg + 1))
    return x


def main_kernel(
    eta_ref, table_ref, temp_hbm, depth_hbm, zonal_hbm, merid_hbm, back_a, back_b,
    temp_ref, depth_ref, zonal_ref, merid_ref,
    send_a, send_b, land_a, land_b, south_ref, ret_a, ret_b,
    rows_ref, edge_ref, par_ref, res_ref, send_sem, recv_sem, own_sem,
):
    lat, me = lax.axis_index("lat"), lax.axis_index("lev")
    lane = lanes()
    row = lax.broadcasted_iota(jnp.int32, (8, 128), 0)
    other = (1 - lat, me)
    loads = [
        pltpu.make_async_copy(src, dst, own_sem.at[i])
        for i, (src, dst) in enumerate(
            ((depth_hbm, depth_ref), (temp_hbm, temp_ref), (zonal_hbm, zonal_ref), (merid_hbm, merid_ref))
        )
    ]
    for c in loads:
        c.start()

    along = [
        [step * lax.rem(at + d, 4) for d in range(4)]
        for step, at in ((1, lax.rem(me, 4)), (4, lax.rem(me // 4, 4)), (16, me // 16))
    ]
    peers = [along[0][x] + along[1][y] + along[2][z] for x, y, z in OFFSETS]
    barrier = pltpu.get_barrier_semaphore()
    for p in peers:
        pl.semaphore_signal(barrier, inc=1, device_id=(lat, p), device_id_type=MESH)
    pl.semaphore_signal(barrier, inc=1, device_id=other, device_id_type=MESH)

    def copy(src, dst, i, device):
        return pltpu.make_async_remote_copy(
            src_ref=src, dst_ref=dst, send_sem=send_sem.at[i], recv_sem=recv_sem.at[i],
            device_id=device, device_id_type=MESH,
        )

    def scatter(src, dst, i):
        for p in peers:
            copy(src.at[p], dst.at[me], i, (lat, p)).start()

    def everyone(src, dst, i):
        return copy(src.at[pl.ds(0, N - 1)], dst.at[pl.ds(0, N - 1)], i, other)

    refs = (temp_ref, depth_ref, zonal_ref, merid_ref)

    def spread(fields):
        def one(chunk, _):
            for field in fields:
                for level in range(2):
                    at = pl.ds(pl.multiple_of(128 * chunk, 128), 128)
                    rows_ref[2 * field + level, chunk] = refs[field][:, level, at]
            return 0

        lax.fori_loop(0, CHUNKS, one, 0, unroll=5)

    def pack(pieces, out):
        for c in range(N):
            regs = [None] * REGS_F
            for field, level, offset in pieces:
                extra = 1 if field == 1 else 0
                chunk, start = divmod((BLK * c - extra) % LON, 128)
                x = rows_ref[2 * field + level, chunk]
                if start + BLK + extra > 128:
                    x = jnp.where(lane >= start, x, rows_ref[2 * field + level, (chunk + 1) % CHUNKS])
                place(regs, roll_lanes(x, offset - start), offset, BLK + extra, lane)
            for r in range(REGS_F):
                out[c, :, 128 * r : 128 * (r + 1)] = regs[r]

    loads[0].wait()
    loads[1].wait()
    spread((0, 1))
    pack(FWD_A, send_a)
    land_a[me] = send_a[me]
    pl.semaphore_wait(barrier, N)
    scatter(send_a, land_a, 0)
    loads[2].wait()
    loads[3].wait()
    spread((2, 3))
    pack(FWD_B, send_b)
    land_b[me] = send_b[me]
    scatter(send_b, land_b, 1)

    top = jnp.full((8, 128), TOP, F32)
    zero = jnp.zeros((8, 128), F32)
    for kind in range(3):
        for p in range(6):
            par_ref[kind, LEV, p] = zero

    def piece(ref, s, offset, width, shift):
        def load(r):
            return ref[s, :, 128 * r : 128 * (r + 1)]

        return roll_lanes(take(load, offset, width, lane), shift - offset)

    def power(x):
        return jnp.exp(KAPPA * jnp.log(x))

    def coefficients(kind, s, above, left, right, q, edge, h):
        bend = q - 0.5 * (left + right)
        par_ref[kind, s, 0] = edge
        par_ref[kind, s, 1] = 1.0 / h
        par_ref[kind, s, 2] = h * left
        par_ref[kind, s, 3] = h * (0.5 * (right - left) + 3.0 * bend)
        par_ref[kind, s, 4] = -2.0 * (h * bend)
        par_ref[kind, s, 5] = above
        return above + h * q

    def layer(kind, s, state, edge_next, q_next, first):
        above, left, q, edge, h, lower = state
        h_next = edge_next - lower
        if first:
            return zero, q_next, q_next, lower, h_next, edge_next
        right = (h_next * q + h * q_next) / (h + h_next)
        above = coefficients(kind, s - 1, above, left, right, q, edge, h)
        return above, right, q_next, lower, h_next, edge_next

    def finish(kind, state):
        above, left, q, edge, h, lower = state
        coefficients(kind, LEV - 1, above, left, q, q, edge, h)
        return lower - TOP

    begin = (zero, zero, zero, zero, zero, top)

    everyone(send_a, land_a, 0).wait_recv()
    share = copy(land_a.at[:, :, pl.ds(0, 256)], south_ref, 4, other)
    share.start()

    def gather_a(s, carry, first=False):
        state, press, work = carry
        for level in range(2):
            x = piece(land_a, s, 91 * level, BLK + 1, -1)
            q = piece(land_a, s, 182 + 90 * level, BLK, 0)
            edge = state[5] + x
            state = layer(0, 2 * s + level, state, edge, q, first and level == 0)
            edge_ref[2 * s + level] = edge
            res_ref[0, 2 * s + level] = work
            below = power(edge)
            work = work + q * (below - press)
            press = below
        return state, press, work

    carry = gather_a(0, (begin, power(top), zero), True)
    state, _, work = lax.fori_loop(1, N, gather_a, carry, unroll=3)
    depth = finish(0, state)

    def remap(kinds, spans):
        def target(k, carry):
            eta0, eta1 = eta_ref[k], eta_ref[k + 1]
            out = []
            for kind, span, before in zip(kinds, spans, carry):
                lower = TOP + eta1 * span
                first = table_ref[kind, 0, k]
                count = table_ref[kind, 1, k]
                mass = par_ref[kind, first, 5]
                for m in range(3):
                    s = first if m == 0 else jnp.where(m < count, first + m, LEV)
                    x = jnp.clip((lower - par_ref[kind, s, 0]) * par_ref[kind, s, 1], 0.0, 1.0)
                    mass = mass + x * (par_ref[kind, s, 2] + x * (par_ref[kind, s, 3] + x * par_ref[kind, s, 4]))
                res_ref[1 + kind, k] = (mass - before) / ((eta1 - eta0) * span)
                out.append(mass)
            return tuple(out)

        lax.fori_loop(0, LEV, target, (zero,) * len(kinds), unroll=4)

    def send_back(pieces, regs_of, out):
        def build(s, _):
            regs = [None] * regs_of
            for field, level, offset in pieces:
                if field == 2:
                    x = depth
                else:
                    x = res_ref[(0, 1, None, 2, 3)[field], 2 * s + level]
                if field == 0:
                    x = work - x
                place(regs, roll_lanes(x, offset), offset, BLK, lane)
            for r in range(regs_of):
                out[s, :, 128 * r : 128 * (r + 1)] = regs[r]
            return 0

        lax.fori_loop(0, N, build, 0, unroll=4)

    remap((0,), (depth,))
    send_back(BACK_A, REGS_A, ret_a)
    scatter(ret_a, back_a, 2)
    back_a[me] = ret_a[me]

    share.wait_recv()
    everyone(send_b, land_b, 1).wait_recv()
    own_first = jnp.logical_and(row == 0, lat == 0)

    def gather_b(s, carry, first=False):
        south, zonal, merid = carry
        for level in range(2):
            at = 2 * s + level
            south = south + piece(south_ref, s, 91 * level, BLK + 1, -1)
            own = edge_ref[at]
            before = pltpu.roll(jnp.where(row == 7, south, own), 1, axis=0)
            edge = jnp.where(own_first, own, 0.5 * (before + own))
            zonal = layer(1, at, zonal, edge, piece(land_b, s, 90 * level, BLK, 0), first and level == 0)
            edge = 0.5 * (roll_lanes(own, 1) + own)
            merid = layer(2, at, merid, edge, piece(land_b, s, 180 + 90 * level, BLK, 0), first and level == 0)
        return south, zonal, merid

    carry = gather_b(0, (top, begin, begin), True)
    _, zonal, merid = lax.fori_loop(1, N, gather_b, carry, unroll=3)
    remap((1, 2), (finish(1, zonal), finish(2, merid)))
    send_back(BACK_B, REGS_B, ret_b)
    scatter(ret_b, back_b, 3)
    back_b[me] = ret_b[me]

    everyone(send_a, land_a, 0).wait_send()
    everyone(send_b, land_b, 1).wait_send()
    share.wait_send()
    everyone(ret_a, back_a, 2).wait()
    everyone(ret_b, back_b, 3).wait()


def unpack_kernel(
    eta_ref, back_a, back_b, surface_hbm, temp_hbm, depth_hbm, zonal_hbm, merid_hbm, phi_hbm,
    surface_ref, out_ref, in_sem, out_sem,
):
    lane = lanes()
    me = lax.axis_index("lev")
    steps = [eta_ref[2 * me + level + 1] - eta_ref[2 * me + level] for level in range(2)]
    surface = pltpu.make_async_copy(surface_hbm, surface_ref, in_sem)
    surface.start()
    outs = (phi_hbm, temp_hbm, depth_hbm, zonal_hbm, merid_hbm)
    stores = [pltpu.make_async_copy(out_ref.at[i], outs[i], out_sem.at[i]) for i in range(5)]
    order = BACK_A[2:] + BACK_B + BACK_A[:2]
    for field, level, offset in order:
        if (field, level) == (0, 0):
            surface.wait()
        recv_ref = back_b if field > 2 else back_a
        current = None
        for c in range(N):

            def load(r):
                return recv_ref[c, :, 128 * r : 128 * (r + 1)]

            chunk, start = divmod(BLK * c, 128)
            x = roll_lanes(take(load, offset, BLK, lane), start - offset)
            current = x if start == 0 else jnp.where(lane >= start, x, current)
            if start + BLK < 128:
                continue
            at = slice(128 * chunk, 128 * (chunk + 1))
            if field == 2:
                for k in range(2):
                    out_ref[2, :, k, at] = steps[k] * current
            else:
                y = current + surface_ref[:, at] if field == 0 else current
                out_ref[field, :, level, at] = y
            current = x
        if field == 2 or level == 1:
            stores[field].start()
    for c in stores:
        c.wait()


ANY = pl.BlockSpec(memory_space=pl.ANY)
VMEM = pl.BlockSpec(memory_space=pltpu.VMEM)
SMEM = pl.BlockSpec(memory_space=pltpu.SMEM)


def on_device(temp, depth, zonal, merid, surface, eta, intersection):
    table = intersection[:, :, :, 0, 0]
    backs = pl.pallas_call(
        main_kernel,
        out_shape=[
            pltpu.VMEM((N, 8, 128 * REGS_A), F32),
            pltpu.VMEM((N, 8, 128 * REGS_B), F32),
        ],
        in_specs=[SMEM, SMEM] + [ANY] * 4,
        out_specs=[VMEM] * 2,
        scratch_shapes=[
            *[pltpu.VMEM((8, 2, LON), F32)] * 4,
            *[pltpu.VMEM((N, 8, 128 * REGS_F), F32)] * 4,
            pltpu.VMEM((N, 8, 256), F32),
            pltpu.VMEM((N, 8, 128 * REGS_A), F32),
            pltpu.VMEM((N, 8, 128 * REGS_B), F32),
            pltpu.VMEM((8, CHUNKS, 8, 128), F32),
            pltpu.VMEM((LEV, 8, 128), F32),
            pltpu.VMEM((3, LEV + 1, 6, 8, 128), F32),
            pltpu.VMEM((4, LEV, 8, 128), F32),
            pltpu.SemaphoreType.DMA((5,)),
            pltpu.SemaphoreType.DMA((5,)),
            pltpu.SemaphoreType.DMA((4,)),
        ],
        compiler_params=pltpu.CompilerParams(collective_id=0, has_side_effects=True),
        name="remap",
    )(eta, table, temp, depth, zonal, merid)
    outs = pl.pallas_call(
        unpack_kernel,
        out_shape=[jax.ShapeDtypeStruct((8, 2, LON), F32)] * 5,
        in_specs=[SMEM, VMEM, VMEM, ANY],
        out_specs=[ANY] * 5,
        scratch_shapes=[
            pltpu.VMEM((8, LON), F32),
            pltpu.VMEM((5, 8, 2, LON), F32),
            pltpu.SemaphoreType.DMA,
            pltpu.SemaphoreType.DMA((5,)),
        ],
        name="unpack",
    )(eta, *(pltpu.with_memory_space_constraint(x, pltpu.VMEM) for x in backs), surface)
    return tuple(outs)


def solution(mesh):
    shards = P("lat", "lev", None)
    return jax.shard_map(
        on_device,
        mesh=mesh,
        in_specs=(shards,) * 4 + (P("lat", None), P(), P(None, None, None, "lat", "lev")),
        out_specs=(shards,) * 5,
        check_vma=False,
    )
```

```python
import functools

import jax
import jax.numpy as jnp
from jax import lax
from jax.experimental import pallas as pl
from jax.experimental.pallas import tpu as pltpu
from jax.sharding import PartitionSpec as P

TOP = 0.2
KAPPA = 0.2857
LEV = 128
LON = 5760
BLK = 90
N = 64
CHUNKS = LON // 128
F32 = jnp.float32

FWD_A = ((1, 0, 0), (1, 1, 91), (0, 0, 182), (0, 1, 272))
FWD_B = ((2, 0, 0), (2, 1, 90), (3, 0, 180), (3, 1, 270))
BACK_A = ((0, 0, 0), (0, 1, 90), (1, 0, 180), (1, 1, 270))
BACK_B = ((3, 0, 0), (3, 1, 90), (4, 0, 180), (4, 1, 270))
REGS_F = REGS_A = REGS_B = 3
FREE = 24
MESH = pl.DeviceIdType.MESH


def offsets():
    every = [(x, y, z) for z in range(4) for y in range(4) for x in range(4)][1:]
    order = []
    for d in sorted(every, key=lambda d: -sum(min(v, 4 - v) for v in d)):
        for r in range(3):
            e = d[r:] + d[:r]
            for f in (e, tuple((4 - v) % 4 for v in e)):
                if f not in order:
                    order.append(f)
    return order


OFFSETS = offsets()


def lanes():
    return lax.broadcasted_iota(jnp.int32, (8, 128), 1)


def roll_lanes(x, shift):
    shift = shift % 128
    return x if isinstance(shift, int) and shift == 0 else pltpu.roll(x, shift, axis=1)


def place(regs, piece, offset, width, lane):
    reg, start = divmod(offset, 128)
    regs[reg] = piece if regs[reg] is None else jnp.where(lane >= start, piece, regs[reg])
    if start + width > 128:
        regs[reg + 1] = piece


def take(load, offset, width, lane):
    reg, start = divmod(offset, 128)
    x = load(reg)
    if start + width > 128:
        x = jnp.where(lane >= start, x, load(reg + 1))
    return x


def main_kernel(
    eta_ref, table_ref, temp_hbm, depth_hbm, zonal_hbm, merid_hbm, back_a, back_b, back_t,
    temp_ref, depth_ref, zonal_ref, merid_ref,
    send_a, send_b, land_a, land_b, south_ref, ret_a, ret_b, ret_t,
    rows_ref, edge_ref, par_ref, res_ref, send_sem, recv_sem, own_sem,
):
    lat, me = lax.axis_index("lat"), lax.axis_index("lev")
    lane = lanes()
    row = lax.broadcasted_iota(jnp.int32, (8, 128), 0)
    other = (1 - lat, me)
    loads = [
        pltpu.make_async_copy(src, dst, own_sem.at[i])
        for i, (src, dst) in enumerate(
            ((depth_hbm, depth_ref), (temp_hbm, temp_ref), (zonal_hbm, zonal_ref), (merid_hbm, merid_ref))
        )
    ]
    for c in loads:
        c.start()

    along = [
        [step * lax.rem(at + d, 4) for d in range(4)]
        for step, at in ((1, lax.rem(me, 4)), (4, lax.rem(me // 4, 4)), (16, me // 16))
    ]
    peers = [along[0][x] + along[1][y] + along[2][z] for x, y, z in OFFSETS]
    barrier = pltpu.get_barrier_semaphore()
    for p in peers:
        pl.semaphore_signal(barrier, inc=1, device_id=(lat, p), device_id_type=MESH)
    pl.semaphore_signal(barrier, inc=1, device_id=other, device_id_type=MESH)

    def copy(src, dst, i, device):
        return pltpu.make_async_remote_copy(
            src_ref=src, dst_ref=dst, send_sem=send_sem.at[i], recv_sem=recv_sem.at[i],
            device_id=device, device_id_type=MESH,
        )

    def scatter(src, dst, i):
        for p in peers:
            copy(src.at[p], dst.at[me], i, (lat, p)).start()

    def everyone(src, dst, i):
        return copy(src.at[pl.ds(0, N - 1)], dst.at[pl.ds(0, N - 1)], i, other)

    refs = (temp_ref, depth_ref, zonal_ref, merid_ref)

    def spread(fields):
        def one(chunk, _):
            for field in fields:
                for level in range(2):
                    at = pl.ds(pl.multiple_of(128 * chunk, 128), 128)
                    rows_ref[2 * field + level, chunk] = refs[field][:, level, at]
            return 0

        lax.fori_loop(0, CHUNKS, one, 0, unroll=5)

    def pack(pieces, out):
        for c in range(N):
            regs = [None] * REGS_F
            for field, level, offset in pieces:
                extra = 1 if field == 1 else 0
                chunk, start = divmod((BLK * c - extra) % LON, 128)
                x = rows_ref[2 * field + level, chunk]
                if start + BLK + extra > 128:
                    x = jnp.where(lane >= start, x, rows_ref[2 * field + level, (chunk + 1) % CHUNKS])
                place(regs, roll_lanes(x, offset - start), offset, BLK + extra, lane)
            for r in range(REGS_F):
                out[c, :, 128 * r : 128 * (r + 1)] = regs[r]

    loads[0].wait()
    loads[1].wait()
    spread((0, 1))
    pack(FWD_A, send_a)
    land_a[me] = send_a[me]
    pl.semaphore_wait(barrier, N)
    scatter(send_a, land_a, 0)
    loads[2].wait()
    loads[3].wait()
    spread((2, 3))
    pack(FWD_B, send_b)
    land_b[me] = send_b[me]
    scatter(send_b, land_b, 1)

    top = jnp.full((8, 128), TOP, F32)
    zero = jnp.zeros((8, 128), F32)
    for kind in range(3):
        for p in range(6):
            par_ref[kind, LEV, p] = zero

    def piece(ref, s, offset, width, shift):
        def load(r):
            return ref[s, :, 128 * r : 128 * (r + 1)]

        return roll_lanes(take(load, offset, width, lane), shift - offset)

    def power(x):
        return jnp.exp(KAPPA * jnp.log(x))

    def coefficients(kind, s, above, left, right, q, edge, h):
        bend = q - 0.5 * (left + right)
        par_ref[kind, s, 0] = edge
        par_ref[kind, s, 1] = 1.0 / h
        par_ref[kind, s, 2] = h * left
        par_ref[kind, s, 3] = h * (0.5 * (right - left) + 3.0 * bend)
        par_ref[kind, s, 4] = -2.0 * (h * bend)
        par_ref[kind, s, 5] = above
        return above + h * q

    def layer(kind, s, state, edge_next, q_next, first):
        above, left, q, edge, h, lower = state
        h_next = edge_next - lower
        if first:
            return zero, q_next, q_next, lower, h_next, edge_next
        right = (h_next * q + h * q_next) / (h + h_next)
        above = coefficients(kind, s - 1, above, left, right, q, edge, h)
        return above, right, q_next, lower, h_next, edge_next

    def finish(kind, state):
        above, left, q, edge, h, lower = state
        coefficients(kind, LEV - 1, above, left, q, q, edge, h)
        return lower - TOP

    begin = (zero, zero, zero, zero, zero, top)

    everyone(send_a, land_a, 0).wait_recv()
    share = copy(land_a.at[:, :, pl.ds(0, 256)], south_ref, 4, other)
    share.start()

    def gather_a(s, carry, first=False):
        state, press, work = carry
        for level in range(2):
            x = piece(land_a, s, 91 * level, BLK + 1, -1)
            q = piece(land_a, s, 182 + 90 * level, BLK, 0)
            edge = state[5] + x
            state = layer(0, 2 * s + level, state, edge, q, first and level == 0)
            edge_ref[2 * s + level] = edge
            res_ref[0, 2 * s + level] = work
            below = power(edge)
            work = work + q * (below - press)
            press = below
        return state, press, work

    carry = gather_a(0, (begin, power(top), zero), True)
    state, _, work = lax.fori_loop(1, N, gather_a, carry, unroll=3)
    depth = finish(0, state)
    rest = roll_lanes(depth, -2 * FREE)
    rest = jnp.where(lane < 64, rest, roll_lanes(pltpu.roll(rest, 4, axis=0), 64))
    ret_t[...] = rest[0:4]

    def remap(kinds, spans):
        def target(k, carry):
            eta0, eta1 = eta_ref[k], eta_ref[k + 1]
            out = []
            for kind, span, before in zip(kinds, spans, carry):
                lower = TOP + eta1 * span
                first = table_ref[kind, 0, k]
                count = table_ref[kind, 1, k]
                mass = par_ref[kind, first, 5]
                for m in range(3):
                    s = first if m == 0 else jnp.where(m < count, first + m, LEV)
                    x = jnp.clip((lower - par_ref[kind, s, 0]) * par_ref[kind, s, 1], 0.0, 1.0)
                    mass = mass + x * (par_ref[kind, s, 2] + x * (par_ref[kind, s, 3] + x * par_ref[kind, s, 4]))
                res_ref[1 + kind, k] = (mass - before) / ((eta1 - eta0) * span)
                out.append(mass)
            return tuple(out)

        lax.fori_loop(0, LEV, target, (zero,) * len(kinds), unroll=4)

    def send_back(pieces, regs_of, out, extra):
        def build(s, _):
            regs = [None] * regs_of
            for field, level, offset in pieces:
                x = res_ref[(0, 1, None, 2, 3)[field], 2 * s + level]
                if field == 0:
                    x = work - x
                place(regs, roll_lanes(x, offset), offset, BLK, lane)
            regs[-1] = jnp.where(lane >= 128 - FREE, extra, regs[-1])
            for r in range(regs_of):
                out[s, :, 128 * r : 128 * (r + 1)] = regs[r]
            return 0

        lax.fori_loop(0, N, build, 0, unroll=4)

    back_t[me] = ret_t[...]
    for p in peers:
        copy(ret_t, back_t.at[me], 5, (lat, p)).start()
    remap((0,), (depth,))
    send_back(BACK_A, REGS_A, ret_a, roll_lanes(depth, -FREE))
    scatter(ret_a, back_a, 2)
    back_a[me] = ret_a[me]

    share.wait_recv()
    everyone(send_b, land_b, 1).wait_recv()
    own_first = jnp.logical_and(row == 0, lat == 0)

    def gather_b(s, carry, first=False):
        south, zonal, merid = carry
        for level in range(2):
            at = 2 * s + level
            south = south + piece(south_ref, s, 91 * level, BLK + 1, -1)
            own = edge_ref[at]
            before = pltpu.roll(jnp.where(row == 7, south, own), 1, axis=0)
            edge = jnp.where(own_first, own, 0.5 * (before + own))
            zonal = layer(1, at, zonal, edge, piece(land_b, s, 90 * level, BLK, 0), first and level == 0)
            edge = 0.5 * (roll_lanes(own, 1) + own)
            merid = layer(2, at, merid, edge, piece(land_b, s, 180 + 90 * level, BLK, 0), first and level == 0)
        return south, zonal, merid

    carry = gather_b(0, (top, begin, begin), True)
    _, zonal, merid = lax.fori_loop(1, N, gather_b, carry, unroll=3)
    remap((1, 2), (finish(1, zonal), finish(2, merid)))
    send_back(BACK_B, REGS_B, ret_b, roll_lanes(depth, -2 * FREE))
    scatter(ret_b, back_b, 3)
    back_b[me] = ret_b[me]

    everyone(send_a, land_a, 0).wait_send()
    everyone(send_b, land_b, 1).wait_send()
    share.wait_send()
    everyone(ret_a, back_a, 2).wait()
    everyone(ret_b, back_b, 3).wait()
    rests = copy(back_t.at[pl.ds(0, N - 1)], back_t.at[pl.ds(0, N - 1)], 5, other)
    rests.wait()


def unpack_kernel(
    eta_ref, back_a, back_b, back_t, surface_hbm, temp_hbm, depth_hbm, zonal_hbm, merid_hbm, phi_hbm,
    surface_ref, span_ref, out_ref, in_sem, out_sem,
):
    lane = lanes()
    me = lax.axis_index("lev")
    steps = [eta_ref[2 * me + level + 1] - eta_ref[2 * me + level] for level in range(2)]
    surface = pltpu.make_async_copy(surface_hbm, surface_ref, in_sem)
    surface.start()
    outs = (phi_hbm, temp_hbm, depth_hbm, zonal_hbm, merid_hbm)
    stores = [pltpu.make_async_copy(out_ref.at[i], outs[i], out_sem.at[i]) for i in range(5)]
    row = lax.broadcasted_iota(jnp.int32, (8, 128), 0)

    def spans(g, _):
        pair = back_t[g]
        swapped = pltpu.roll(pair, 4, axis=0)
        for k, (upper, lower) in enumerate(((pair, swapped), (swapped, pair))):
            first = roll_lanes(back_a[2 * g + k, :, 256:384], FREE)
            second = roll_lanes(back_b[2 * g + k, :, 256:384], 2 * FREE)
            rest = jnp.where(row < 4, roll_lanes(upper, 2 * FREE), roll_lanes(lower, 2 * FREE + 64))
            x = jnp.where(lane < FREE, first, jnp.where(lane < 2 * FREE, second, rest))
            span_ref[2 * g + k] = x
        return 0

    lax.fori_loop(0, N // 2, spans, 0, unroll=16)
    order = BACK_A[2:] + BACK_B + ((2, 0, 0),) + BACK_A[:2]
    for field, level, offset in order:
        if (field, level) == (0, 0):
            surface.wait()
        recv_ref = back_b if field > 2 else back_a
        current = None
        for c in range(N):

            def load(r):
                return recv_ref[c, :, 128 * r : 128 * (r + 1)]

            chunk, start = divmod(BLK * c, 128)
            x = span_ref[c] if field == 2 else take(load, offset, BLK, lane)
            x = roll_lanes(x, start - offset)
            current = x if start == 0 else jnp.where(lane >= start, x, current)
            if start + BLK < 128:
                continue
            at = slice(128 * chunk, 128 * (chunk + 1))
            if field == 2:
                for k in range(2):
                    out_ref[2, :, k, at] = steps[k] * current
            else:
                y = current + surface_ref[:, at] if field == 0 else current
                out_ref[field, :, level, at] = y
            current = x
        if field == 2 or level == 1:
            stores[field].start()
    for c in stores:
        c.wait()


ANY = pl.BlockSpec(memory_space=pl.ANY)
VMEM = pl.BlockSpec(memory_space=pltpu.VMEM)
SMEM = pl.BlockSpec(memory_space=pltpu.SMEM)


def on_device(temp, depth, zonal, merid, surface, eta, intersection):
    table = intersection[:, :, :, 0, 0]
    backs = pl.pallas_call(
        main_kernel,
        out_shape=[
            pltpu.VMEM((N, 8, 128 * REGS_A), F32),
            pltpu.VMEM((N, 8, 128 * REGS_B), F32),
            pltpu.VMEM((N, 4, 128), F32),
        ],
        in_specs=[SMEM, SMEM] + [ANY] * 4,
        out_specs=[VMEM] * 3,
        scratch_shapes=[
            *[pltpu.VMEM((8, 2, LON), F32)] * 4,
            *[pltpu.VMEM((N, 8, 128 * REGS_F), F32)] * 4,
            pltpu.VMEM((N, 8, 256), F32),
            pltpu.VMEM((N, 8, 128 * REGS_A), F32),
            pltpu.VMEM((N, 8, 128 * REGS_B), F32),
            pltpu.VMEM((4, 128), F32),
            pltpu.VMEM((8, CHUNKS, 8, 128), F32),
            pltpu.VMEM((LEV, 8, 128), F32),
            pltpu.VMEM((3, LEV + 1, 6, 8, 128), F32),
            pltpu.VMEM((4, LEV, 8, 128), F32),
            pltpu.SemaphoreType.DMA((6,)),
            pltpu.SemaphoreType.DMA((6,)),
            pltpu.SemaphoreType.DMA((4,)),
        ],
        compiler_params=pltpu.CompilerParams(collective_id=0, has_side_effects=True),
        name="remap",
    )(eta, table, temp, depth, zonal, merid)
    backs = [backs[0], backs[1], backs[2].reshape(N // 2, 8, 128)]
    outs = pl.pallas_call(
        unpack_kernel,
        out_shape=[jax.ShapeDtypeStruct((8, 2, LON), F32)] * 5,
        in_specs=[SMEM, VMEM, VMEM, VMEM, ANY],
        out_specs=[ANY] * 5,
        scratch_shapes=[
            pltpu.VMEM((8, LON), F32),
            pltpu.VMEM((N, 8, 128), F32),
            pltpu.VMEM((5, 8, 2, LON), F32),
            pltpu.SemaphoreType.DMA,
            pltpu.SemaphoreType.DMA((5,)),
        ],
        name="unpack",
    )(eta, *(pltpu.with_memory_space_constraint(x, pltpu.VMEM) for x in backs), surface)
    return tuple(outs)


def solution(mesh):
    shards = P("lat", "lev", None)
    return jax.shard_map(
        on_device,
        mesh=mesh,
        in_specs=(shards,) * 4 + (P("lat", None), P(), P(None, None, None, "lat", "lev")),
        out_specs=(shards,) * 5,
        check_vma=False,
    )
```

```python
import functools

import jax
import jax.numpy as jnp
from jax import lax
from jax.experimental import pallas as pl
from jax.experimental.pallas import tpu as pltpu
from jax.sharding import PartitionSpec as P

TOP = 0.2
KAPPA = 0.2857
LEV = 128
LON = 5760
BLK = 90
N = 64
CHUNKS = LON // 128
F32 = jnp.float32

FWD_A = ((1, 0, 0), (1, 1, 91), (0, 0, 182), (0, 1, 272))
FWD_B = ((2, 0, 0), (2, 1, 90), (3, 0, 180), (3, 1, 270))
BACK_A = ((0, 0, 0), (0, 1, 90), (1, 0, 180), (1, 1, 270))
BACK_B = ((3, 0, 0), (3, 1, 90), (4, 0, 180), (4, 1, 270))
REGS_F = REGS_A = REGS_B = 3
FREE = 24
MESH = pl.DeviceIdType.MESH


def offsets():
    every = [(x, y, z) for z in range(4) for y in range(4) for x in range(4)][1:]
    order = []
    for d in sorted(every, key=lambda d: -sum(min(v, 4 - v) for v in d)):
        for r in range(3):
            e = d[r:] + d[:r]
            for f in (e, tuple((4 - v) % 4 for v in e)):
                if f not in order:
                    order.append(f)
    return order


OFFSETS = offsets()


def lanes():
    return lax.broadcasted_iota(jnp.int32, (8, 128), 1)


def roll_lanes(x, shift):
    shift = shift % 128
    return x if isinstance(shift, int) and shift == 0 else pltpu.roll(x, shift, axis=1)


def place(regs, piece, offset, width, lane):
    reg, start = divmod(offset, 128)
    regs[reg] = piece if regs[reg] is None else jnp.where(lane >= start, piece, regs[reg])
    if start + width > 128:
        regs[reg + 1] = piece


def take(load, offset, width, lane):
    reg, start = divmod(offset, 128)
    x = load(reg)
    if start + width > 128:
        x = jnp.where(lane >= start, x, load(reg + 1))
    return x


def main_kernel(
    eta_ref, table_ref, temp_hbm, depth_hbm, zonal_hbm, merid_hbm, back_a, back_b, back_t,
    temp_ref, depth_ref, zonal_ref, merid_ref,
    send_a, send_b, land_a, land_b, south_ref, ret_a, ret_b, ret_t,
    rows_ref, edge_ref, par_ref, res_ref, send_sem, recv_sem, own_sem,
):
    lat, me = lax.axis_index("lat"), lax.axis_index("lev")
    lane = lanes()
    row = lax.broadcasted_iota(jnp.int32, (8, 128), 0)
    other = (1 - lat, me)
    loads = [
        pltpu.make_async_copy(src, dst, own_sem.at[i])
        for i, (src, dst) in enumerate(
            ((depth_hbm, depth_ref), (temp_hbm, temp_ref), (zonal_hbm, zonal_ref), (merid_hbm, merid_ref))
        )
    ]
    for c in loads[:2]:
        c.start()

    along = [
        [step * lax.rem(at + d + 2 * d * lat, 4) for d in range(4)]
        for step, at in ((1, lax.rem(me, 4)), (4, lax.rem(me // 4, 4)), (16, me // 16))
    ]
    peers = [along[0][x] + along[1][y] + along[2][z] for x, y, z in OFFSETS]
    barrier = pltpu.get_barrier_semaphore()
    for p in peers:
        pl.semaphore_signal(barrier, inc=1, device_id=(lat, p), device_id_type=MESH)
    pl.semaphore_signal(barrier, inc=1, device_id=other, device_id_type=MESH)
    for c in loads[2:]:
        c.start()

    def copy(src, dst, i, device):
        return pltpu.make_async_remote_copy(
            src_ref=src, dst_ref=dst, send_sem=send_sem.at[i], recv_sem=recv_sem.at[i],
            device_id=device, device_id_type=MESH,
        )

    def scatter(src, dst, i):
        for p in peers:
            copy(src.at[p], dst.at[me], i, (lat, p)).start()

    def everyone(src, dst, i):
        return copy(src.at[pl.ds(0, N - 1)], dst.at[pl.ds(0, N - 1)], i, other)

    refs = (temp_ref, depth_ref, zonal_ref, merid_ref)

    def spread(fields):
        def one(chunk, _):
            for field in fields:
                for level in range(2):
                    at = pl.ds(pl.multiple_of(128 * chunk, 128), 128)
                    rows_ref[2 * field + level, chunk] = refs[field][:, level, at]
            return 0

        lax.fori_loop(0, CHUNKS, one, 0, unroll=9)

    def pack(pieces, out):
        for c in range(N):
            regs = [None] * REGS_F
            for field, level, offset in pieces:
                extra = 1 if field == 1 else 0
                chunk, start = divmod((BLK * c - extra) % LON, 128)
                x = rows_ref[2 * field + level, chunk]
                if start + BLK + extra > 128:
                    x = jnp.where(lane >= start, x, rows_ref[2 * field + level, (chunk + 1) % CHUNKS])
                place(regs, roll_lanes(x, offset - start), offset, BLK + extra, lane)
            for r in range(REGS_F):
                out[c, :, 128 * r : 128 * (r + 1)] = regs[r]

    loads[0].wait()
    spread((1,))
    loads[1].wait()
    spread((0,))
    pack(FWD_A, send_a)
    land_a[me] = send_a[me]
    pl.semaphore_wait(barrier, N)
    scatter(send_a, land_a, 0)
    loads[2].wait()
    loads[3].wait()
    spread((2, 3))
    pack(FWD_B, send_b)
    land_b[me] = send_b[me]
    scatter(send_b, land_b, 1)

    top = jnp.full((8, 128), TOP, F32)
    zero = jnp.zeros((8, 128), F32)
    for kind in range(3):
        for p in range(6):
            par_ref[kind, LEV, p] = zero

    def piece(ref, s, offset, width, shift):
        def load(r):
            return ref[s, :, 128 * r : 128 * (r + 1)]

        return roll_lanes(take(load, offset, width, lane), shift - offset)

    def power(x):
        return jnp.exp(KAPPA * jnp.log(x))

    def coefficients(kind, s, above, left, right, q, edge, h):
        bend = q - 0.5 * (left + right)
        par_ref[kind, s, 0] = edge
        par_ref[kind, s, 1] = 1.0 / h
        par_ref[kind, s, 2] = h * left
        par_ref[kind, s, 3] = h * (0.5 * (right - left) + 3.0 * bend)
        par_ref[kind, s, 4] = -2.0 * (h * bend)
        par_ref[kind, s, 5] = above
        return above + h * q

    def layer(kind, s, state, edge_next, q_next, first):
        above, left, q, edge, h, lower = state
        h_next = edge_next - lower
        if first:
            return zero, q_next, q_next, lower, h_next, edge_next
        right = (h_next * q + h * q_next) / (h + h_next)
        above = coefficients(kind, s - 1, above, left, right, q, edge, h)
        return above, right, q_next, lower, h_next, edge_next

    def finish(kind, state):
        above, left, q, edge, h, lower = state
        coefficients(kind, LEV - 1, above, left, q, q, edge, h)
        return lower - TOP

    begin = (zero, zero, zero, zero, zero, top)

    everyone(send_a, land_a, 0).wait_recv()
    share = copy(land_a.at[:, :, pl.ds(0, 256)], south_ref, 4, other)
    share.start()

    def gather_a(s, carry, first=False):
        state, press, work = carry
        for level in range(2):
            x = piece(land_a, s, 91 * level, BLK + 1, -1)
            q = piece(land_a, s, 182 + 90 * level, BLK, 0)
            edge = state[5] + x
            state = layer(0, 2 * s + level, state, edge, q, first and level == 0)
            edge_ref[2 * s + level] = edge
            res_ref[0, 2 * s + level] = work
            below = power(edge)
            work = work + q * (below - press)
            press = below
        return state, press, work

    carry = gather_a(0, (begin, power(top), zero), True)
    state, _, work = lax.fori_loop(1, N, gather_a, carry, unroll=3)
    depth = finish(0, state)
    rest = roll_lanes(depth, -2 * FREE)
    rest = jnp.where(lane < 64, rest, roll_lanes(pltpu.roll(rest, 4, axis=0), 64))
    ret_t[...] = rest[0:4]

    def remap(kinds, spans):
        def target(k, carry):
            eta0, eta1 = eta_ref[k], eta_ref[k + 1]
            out = []
            for kind, span, before in zip(kinds, spans, carry):
                lower = TOP + eta1 * span
                first = table_ref[kind, 0, k]
                count = table_ref[kind, 1, k]
                mass = par_ref[kind, first, 5]
                for m in range(3):
                    s = first if m == 0 else jnp.where(m < count, first + m, LEV)
                    x = jnp.clip((lower - par_ref[kind, s, 0]) * par_ref[kind, s, 1], 0.0, 1.0)
                    mass = mass + x * (par_ref[kind, s, 2] + x * (par_ref[kind, s, 3] + x * par_ref[kind, s, 4]))
                res_ref[1 + kind, k] = (mass - before) / ((eta1 - eta0) * span)
                out.append(mass)
            return tuple(out)

        lax.fori_loop(0, LEV, target, (zero,) * len(kinds), unroll=4)

    def send_back(pieces, regs_of, out, extra):
        def build(s, _):
            regs = [None] * regs_of
            for field, level, offset in pieces:
                x = res_ref[(0, 1, None, 2, 3)[field], 2 * s + level]
                if field == 0:
                    x = work - x
                place(regs, roll_lanes(x, offset), offset, BLK, lane)
            regs[-1] = jnp.where(lane >= 128 - FREE, extra, regs[-1])
            for r in range(regs_of):
                out[s, :, 128 * r : 128 * (r + 1)] = regs[r]
            return 0

        lax.fori_loop(0, N, build, 0, unroll=4)

    back_t[me] = ret_t[...]
    for p in peers:
        copy(ret_t, back_t.at[me], 5, (lat, p)).start()
    remap((0,), (depth,))
    send_back(BACK_A, REGS_A, ret_a, roll_lanes(depth, -FREE))
    scatter(ret_a, back_a, 2)
    back_a[me] = ret_a[me]

    share.wait_recv()
    everyone(send_b, land_b, 1).wait_recv()
    own_first = jnp.logical_and(row == 0, lat == 0)

    def gather_b(s, carry, first=False):
        south, zonal, merid = carry
        for level in range(2):
            at = 2 * s + level
            south = south + piece(south_ref, s, 91 * level, BLK + 1, -1)
            own = edge_ref[at]
            before = pltpu.roll(jnp.where(row == 7, south, own), 1, axis=0)
            edge = jnp.where(own_first, own, 0.5 * (before + own))
            zonal = layer(1, at, zonal, edge, piece(land_b, s, 90 * level, BLK, 0), first and level == 0)
            edge = 0.5 * (roll_lanes(own, 1) + own)
            merid = layer(2, at, merid, edge, piece(land_b, s, 180 + 90 * level, BLK, 0), first and level == 0)
        return south, zonal, merid

    carry = gather_b(0, (top, begin, begin), True)
    _, zonal, merid = lax.fori_loop(1, N, gather_b, carry, unroll=3)
    remap((1, 2), (finish(1, zonal), finish(2, merid)))
    send_back(BACK_B, REGS_B, ret_b, roll_lanes(depth, -2 * FREE))
    scatter(ret_b, back_b, 3)
    back_b[me] = ret_b[me]

    everyone(send_a, land_a, 0).wait_send()
    everyone(send_b, land_b, 1).wait_send()
    share.wait_send()
    everyone(ret_a, back_a, 2).wait()
    everyone(ret_b, back_b, 3).wait()
    rests = copy(back_t.at[pl.ds(0, N - 1)], back_t.at[pl.ds(0, N - 1)], 5, other)
    rests.wait()


def unpack_kernel(
    eta_ref, back_a, back_b, back_t, surface_hbm, temp_hbm, depth_hbm, zonal_hbm, merid_hbm, phi_hbm,
    surface_ref, span_ref, out_ref, in_sem, out_sem,
):
    lane = lanes()
    me = lax.axis_index("lev")
    steps = [eta_ref[2 * me + level + 1] - eta_ref[2 * me + level] for level in range(2)]
    surface = pltpu.make_async_copy(surface_hbm, surface_ref, in_sem)
    surface.start()
    outs = (phi_hbm, temp_hbm, depth_hbm, zonal_hbm, merid_hbm)
    stores = [pltpu.make_async_copy(out_ref.at[i], outs[i], out_sem.at[i]) for i in range(5)]
    row = lax.broadcasted_iota(jnp.int32, (8, 128), 0)

    def spans(g, _):
        pair = back_t[g]
        swapped = pltpu.roll(pair, 4, axis=0)
        for k, (upper, lower) in enumerate(((pair, swapped), (swapped, pair))):
            first = roll_lanes(back_a[2 * g + k, :, 256:384], FREE)
            second = roll_lanes(back_b[2 * g + k, :, 256:384], 2 * FREE)
            rest = jnp.where(row < 4, roll_lanes(upper, 2 * FREE), roll_lanes(lower, 2 * FREE + 64))
            x = jnp.where(lane < FREE, first, jnp.where(lane < 2 * FREE, second, rest))
            span_ref[2 * g + k] = x
        return 0

    lax.fori_loop(0, N // 2, spans, 0, unroll=16)
    order = BACK_A[2:] + BACK_B + ((2, 0, 0),) + BACK_A[:2]
    for field, level, offset in order:
        if (field, level) == (0, 0):
            surface.wait()
        recv_ref = back_b if field > 2 else back_a
        current = None
        for c in range(N):

            def load(r):
                return recv_ref[c, :, 128 * r : 128 * (r + 1)]

            chunk, start = divmod(BLK * c, 128)
            x = span_ref[c] if field == 2 else take(load, offset, BLK, lane)
            x = roll_lanes(x, start - offset)
            current = x if start == 0 else jnp.where(lane >= start, x, current)
            if start + BLK < 128:
                continue
            at = slice(128 * chunk, 128 * (chunk + 1))
            if field == 2:
                for k in range(2):
                    out_ref[2, :, k, at] = steps[k] * current
            else:
                y = current + surface_ref[:, at] if field == 0 else current
                out_ref[field, :, level, at] = y
            current = x
        if field == 2 or level == 1:
            stores[field].start()
    for c in stores:
        c.wait()


ANY = pl.BlockSpec(memory_space=pl.ANY)
VMEM = pl.BlockSpec(memory_space=pltpu.VMEM)
SMEM = pl.BlockSpec(memory_space=pltpu.SMEM)


def on_device(temp, depth, zonal, merid, surface, eta, intersection):
    table = intersection[:, :, :, 0, 0]
    backs = pl.pallas_call(
        main_kernel,
        out_shape=[
            pltpu.VMEM((N, 8, 128 * REGS_A), F32),
            pltpu.VMEM((N, 8, 128 * REGS_B), F32),
            pltpu.VMEM((N, 4, 128), F32),
        ],
        in_specs=[SMEM, SMEM] + [ANY] * 4,
        out_specs=[VMEM] * 3,
        scratch_shapes=[
            *[pltpu.VMEM((8, 2, LON), F32)] * 4,
            *[pltpu.VMEM((N, 8, 128 * REGS_F), F32)] * 4,
            pltpu.VMEM((N, 8, 256), F32),
            pltpu.VMEM((N, 8, 128 * REGS_A), F32),
            pltpu.VMEM((N, 8, 128 * REGS_B), F32),
            pltpu.VMEM((4, 128), F32),
            pltpu.VMEM((8, CHUNKS, 8, 128), F32),
            pltpu.VMEM((LEV, 8, 128), F32),
            pltpu.VMEM((3, LEV + 1, 6, 8, 128), F32),
            pltpu.VMEM((4, LEV, 8, 128), F32),
            pltpu.SemaphoreType.DMA((6,)),
            pltpu.SemaphoreType.DMA((6,)),
            pltpu.SemaphoreType.DMA((4,)),
        ],
        compiler_params=pltpu.CompilerParams(collective_id=0, has_side_effects=True),
        name="remap",
    )(eta, table, temp, depth, zonal, merid)
    backs = [backs[0], backs[1], backs[2].reshape(N // 2, 8, 128)]
    outs = pl.pallas_call(
        unpack_kernel,
        out_shape=[jax.ShapeDtypeStruct((8, 2, LON), F32)] * 5,
        in_specs=[SMEM, VMEM, VMEM, VMEM, ANY],
        out_specs=[ANY] * 5,
        scratch_shapes=[
            pltpu.VMEM((8, LON), F32),
            pltpu.VMEM((N, 8, 128), F32),
            pltpu.VMEM((5, 8, 2, LON), F32),
            pltpu.SemaphoreType.DMA,
            pltpu.SemaphoreType.DMA((5,)),
        ],
        name="unpack",
    )(eta, *(pltpu.with_memory_space_constraint(x, pltpu.VMEM) for x in backs), surface)
    return tuple(outs)


def solution(mesh):
    shards = P("lat", "lev", None)
    return jax.shard_map(
        on_device,
        mesh=mesh,
        in_specs=(shards,) * 4 + (P("lat", None), P(), P(None, None, None, "lat", "lev")),
        out_specs=(shards,) * 5,
        check_vma=False,
    )
```
